32 devices in a mesh: dp: 32 (over z, y, x, core).
Axes of the slice: x: 2, y: 2, z: 4, core: 2. Of those that a mesh axis runs over, the one named last changes fastest.
Arguments:
- attn_grad: bfloat16 [32, 4, 1024, 1024], P('dp')
- attn_weight: float32 [4, 1024, 1024], P(None, 'dp')
- attn_row: float32 [4, 1024], P(None, 'dp')
- attn_col: float32 [4, 1024], replicated
- ffin_grad: bfloat16 [32, 1024, 512], P('dp')
- ffin_weight: float32 [1024, 512], P('dp')
- ffin_row: float32 [1024], P('dp')
- ffin_col: float32 [512], replicated
- ffout_grad: bfloat16 [32, 512, 1024], P('dp')
- ffout_weight: float32 [512, 1024], P('dp')
- ffout_row: float32 [512], P('dp')
- ffout_col: float32 [1024], replicated
- exin_grad: float32 [32, 1024, 512], P('dp')
- exin_weight: float32 [32, 1024, 512], P('dp')
- exin_row: float32 [32, 1024], P('dp')
- exin_col: float32 [32, 512], P('dp')
- exout_grad: float32 [32, 512, 1024], P('dp')
- exout_weight: float32 [32, 512, 1024], P('dp')
- exout_row: float32 [32, 512], P('dp')
- exout_col: float32 [32, 1024], P('dp')
Outputs:
- output 1: float32 [4, 1024, 1024], P(None, 'dp')
- output 2: float32 [4, 1024], P(None, 'dp')
- output 3: float32 [4, 1024], replicated
- output 4: float32 [1024, 512], P('dp')
- output 5: float32 [1024], P('dp')
- output 6: float32 [512], replicated
- output 7: float32 [512, 1024], P('dp')
- output 8: float32 [512], P('dp')
- output 9: float32 [1024], replicated
- output 10: float32 [32, 1024, 512], P('dp')
- output 11: float32 [32, 1024], P('dp')
- output 12: float32 [32, 512], P('dp')
- output 13: float32 [32, 512, 1024], P('dp')
- output 14: float32 [32, 512], P('dp')
- output 15: float32 [32, 1024], P('dp')
All inputs are finite; a program needn't handle non-finite values.
Results may differ from the reference program's by a relative error of at most 0.001.
Values sent between devices are 32-bit elements.
A program may use at most 1 GiB of HBM per device.

```python
import jax
import jax.numpy as jnp

D_MODEL = 1024
D_FF = 512
N_EXPERTS = 32
GROUP_SIZE = 32
OPT_STEP = 10

LEARN_RATE = 0.1
EPS_SQUARE = 1e-30
EPS_SCALE = 1e-3
CLIP_LIMIT = 1.0
BETA_TWO = 1.0 - OPT_STEP ** -0.8


def matrix_scales(key_base, lead_dims, n_rows, n_cols):
    key_row, key_col = jax.random.split(key_base)
    row_drift = jnp.linspace(-0.8, 0.8, n_rows)
    row_scale = jnp.exp(0.5 * jax.random.normal(key_row, lead_dims + (n_rows,)) + row_drift)
    col_scale = jnp.exp(0.5 * jax.random.normal(key_col, lead_dims + (n_cols,)))
    return row_scale[..., :, None] * col_scale[..., None, :]


def local_grads(key_base, lead_dims, n_rows, n_cols):
    key_scale, key_shared, key_dev = jax.random.split(key_base, 3)
    scales = matrix_scales(key_scale, lead_dims, n_rows, n_cols)
    shared = jax.random.normal(key_shared, lead_dims + (n_rows, n_cols))
    per_dev = jax.random.normal(key_dev, (GROUP_SIZE,) + lead_dims + (n_rows, n_cols))
    return ((shared + 0.5 * per_dev) * scales).astype(jnp.bfloat16)


def full_grads(key_base, lead_dims, n_rows, n_cols):
    key_scale, key_val = jax.random.split(key_base)
    scales = matrix_scales(key_scale, lead_dims, n_rows, n_cols)
    return jax.random.normal(key_val, lead_dims + (n_rows, n_cols)) * scales


def weights(key_base, lead_dims, n_rows, n_cols):
    key_val, key_row = jax.random.split(key_base)
    row_drift = jnp.linspace(-0.5, 0.5, n_rows)
    row_scale = jnp.exp(0.3 * jax.random.normal(key_row, lead_dims + (n_rows,)) + row_drift)
    values = jax.random.normal(key_val, lead_dims + (n_rows, n_cols))
    return values * row_scale[..., :, None] * n_rows ** -0.5


def states(key_base, shape):
    return 0.2 * jnp.exp(0.5 * jax.random.normal(key_base, shape))


def matrix_group(key_base, lead_dims, n_rows, n_cols, dense):
    key_grad, key_weight, key_row, key_col = jax.random.split(key_base, 4)
    if dense:
        gradient = local_grads(key_grad, lead_dims, n_rows, n_cols)
    else:
        gradient = full_grads(key_grad, lead_dims, n_rows, n_cols)
    return (gradient, weights(key_weight, lead_dims, n_rows, n_cols),
            states(key_row, lead_dims + (n_rows,)), states(key_col, lead_dims + (n_cols,)))


def setup_inputs(seed: int = 0) -> dict:
    sub_keys = jax.random.split(jax.random.key(seed), 5)
    names = ("attn", "ffin", "ffout", "exin", "exout")
    groups = (
        matrix_group(sub_keys[0], (4,), D_MODEL, D_MODEL, True),
        matrix_group(sub_keys[1], (), D_MODEL, D_FF, True),
        matrix_group(sub_keys[2], (), D_FF, D_MODEL, True),
        matrix_group(sub_keys[3], (N_EXPERTS,), D_MODEL, D_FF, False),
        matrix_group(sub_keys[4], (N_EXPERTS,), D_FF, D_MODEL, False),
    )
    inputs = {}
    for name, group in zip(names, groups):
        inputs[name + "_grad"] = group[0]
        inputs[name + "_weight"] = group[1]
        inputs[name + "_row"] = group[2]
        inputs[name + "_col"] = group[3]
    return inputs


def adafactor(gradient, weight, row_state, col_state):
    square = gradient * gradient + EPS_SQUARE
    row_new = BETA_TWO * row_state + (1.0 - BETA_TWO) * jnp.mean(square, axis=-1)
    col_new = BETA_TWO * col_state + (1.0 - BETA_TWO) * jnp.mean(square, axis=-2)
    row_mean = jnp.mean(row_new, axis=-1, keepdims=True)
    second = row_new[..., :, None] * col_new[..., None, :] / row_mean[..., None]
    update = gradient / jnp.sqrt(second)
    upd_rms = jnp.sqrt(jnp.mean(update * update, axis=(-2, -1), keepdims=True))
    update = update / jnp.maximum(1.0, upd_rms / CLIP_LIMIT)
    w_rms = jnp.sqrt(jnp.mean(weight * weight, axis=(-2, -1), keepdims=True))
    step_size = LEARN_RATE * jnp.maximum(EPS_SCALE, w_rms)
    return weight - step_size * update, row_new, col_new


def reference(attn_grad, attn_weight, attn_row, attn_col, ffin_grad, ffin_weight, ffin_row, ffin_col, ffout_grad, ffout_weight, ffout_row, ffout_col, exin_grad, exin_weight, exin_row, exin_col, exout_grad, exout_weight, exout_row, exout_col):
    attn_new = adafactor(jnp.mean(attn_grad.astype(jnp.float32), axis=0), attn_weight, attn_row, attn_col)
    ffin_new = adafactor(jnp.mean(ffin_grad.astype(jnp.float32), axis=0), ffin_weight, ffin_row, ffin_col)
    ffout_new = adafactor(jnp.mean(ffout_grad.astype(jnp.float32), axis=0), ffout_weight, ffout_row, ffout_col)
    exin_new = adafactor(exin_grad, exin_weight, exin_row, exin_col)
    exout_new = adafactor(exout_grad, exout_weight, exout_row, exout_col)
    return (attn_new[0], attn_new[1], attn_new[2],
            ffin_new[0], ffin_new[1], ffin_new[2],
            ffout_new[0], ffout_new[1], ffout_new[2],
            exin_new[0], exin_new[1], exin_new[2],
            exout_new[0], exout_new[1], exout_new[2])
```

```python
import jax
import jax.numpy as jnp
from jax import lax
from jax.experimental import pallas as pl
from jax.experimental.pallas import tpu as pltpu
from jax.sharding import PartitionSpec as P

OPT_STEP = 10
LEARN_RATE = 0.1
EPS_SQUARE = 1e-30
EPS_SCALE = 1e-3
BETA_TWO = 1.0 - OPT_STEP ** -0.8
KEEP = 1.0 - BETA_TWO
F32 = jnp.float32
BLK_R, BLK_C = 16, 512
N_UNITS = 20
BIT = {"x": 1, "y": 2, "a": 3, "b": 4}

ORDERS = ("xayb", "yaxb") * 10
STEP_UNITS = (
    0, 1, 2, 0, 3, 1, 4, 5, 6, 7, 8, 9, 2, 10, 3, 11, 12, 0, 13, 14, 15, 16, 1, 4,
    17, 5, 18, 19, 2, 3, 1, 0, 6, 2, 4, 7, 5, 0, 3, 1, 8, 4, 6, 0, 9, 2, 1, 7,
    5, 3, 2, 10, 6, 8, 11, 4, 3, 9, 7, 5, 4, 12, 8, 10, 13, 6, 5, 11, 9, 7, 6, 14,
    10, 12, 15, 8, 7, 13, 11, 9, 8, 16, 12, 14, 17, 10, 9, 15, 13, 11, 10, 12, 18, 14, 16, 19,
    11, 12, 17, 15, 13, 14, 16, 18, 13, 17, 14, 19, 15, 16, 18, 17, 15, 19, 16, 18, 17, 19, 18, 19,
)
STEPS = [(u, STEP_UNITS[:n].count(u)) for n, u in enumerate(STEP_UNITS)]

UNITS = [(m, 16 * r, 512 * c) for m in range(4) for r in range(2) for c in range(2)]
UNITS += [(4, 0, 0), (4, 16, 0), (5, 0, 0), (5, 0, 512)]
N_ROWS = (1024, 1024, 1024, 1024, 1024, 512)
N_COLS = (1024, 1024, 1024, 1024, 512, 1024)
LOC_ROWS = (32, 32, 32, 32, 32, 16)
ROW_AT = (0, 32, 64, 96, 128, 160)
GROUP_AT = (0, 8, 16, 24, 32, 36)
MESH = pl.DeviceIdType.MESH


def sum_all(value):
    return jnp.sum(jnp.sum(value, axis=1, keepdims=True), axis=0, keepdims=True)


def dense_kernel(attn_g, ffin_g, ffout_g, attn_w, ffin_w, ffout_w, attn_r, ffin_r, ffout_r, col_in,
                 gsum, row_out, stat_out,
                 raw, stage, r0, r1, r2, r3, r4, msg, rx, tile, rb, ld_sem, s_sem, r_sem, x_sem):
    me = lax.axis_index("dp")
    bits = [(me // 2 ** k) % 2 for k in range(5)]
    partner = [me + (1 - 2 * bits[k]) * 2 ** k for k in range(5)]
    core = bits[0]
    recvs = (r0, r1, r2, r3, r4)

    def source(u):
        m, row, col = UNITS[u]
        if m < 4:
            return attn_g.at[m, :, pl.ds(row, BLK_R), pl.ds(col, BLK_C)]
        ref = ffin_g if m == 4 else ffout_g
        return ref.at[:, pl.ds(row, BLK_R), pl.ds(col, BLK_C)]

    loads = [pltpu.make_async_copy(source(u), raw.at[u], ld_sem.at[u]) for u in range(N_UNITS)]
    for load in loads:
        load.start()

    def dest(order, i):
        return sum(((i // 2 ** (3 - j)) % 2) * 2 ** BIT[order[j]] for j in range(4))

    def copy(u, s):
        order = ORDERS[u]
        if s == 0:
            src, to = stage.at[u], partner[0]
        else:
            keep = sum(bits[BIT[order[j]]] * 2 ** (3 - j) for j in range(s - 1))
            k = BIT[order[s - 1]]
            src = r0.at[u, pl.ds(keep + (1 - bits[k]) * 2 ** (4 - s), 2 ** (4 - s))]
            to = partner[k]
        return pltpu.make_async_remote_copy(
            src_ref=src, dst_ref=recvs[s].at[u], send_sem=s_sem.at[s, u], recv_sem=r_sem.at[s, u],
            device_id=(to,), device_id_type=MESH)

    def block_sum(u, s, i, d):
        total = raw[u, d].astype(F32)
        for j in range(s):
            total = total + recvs[j][u, i % 2 ** (4 - j)]
        return total

    def step(u, s):
        order = ORDERS[u]
        if s == 0:
            loads[u].wait()

            @pl.loop(0, 16)
            def _(i):
                stage[u, i] = raw[u, dest(order, i) + 1 - core].astype(F32)
        else:
            copy(u, s - 1).wait_recv()
            base = sum(bits[BIT[order[j]]] * 2 ** (3 - j) for j in range(min(s - 1, 4)))
            if s == 5:
                gsum[u] = block_sum(u, 5, base, me) * (1.0 / 32.0)
                return
            base = base + (1 - bits[BIT[order[s - 1]]]) * 2 ** (4 - s)

            @pl.loop(0, 2 ** (4 - s))
            def _(n):
                i = base + n
                r0[u, i] = block_sum(u, s, i, dest(order, i) + core)
        copy(u, s).start()

    for u, s in STEPS:
        step(u, s)

    rows_in = (attn_r, attn_r, attn_r, attn_r, ffin_r, ffout_r)
    weights = (attn_w, attn_w, attn_w, attn_w, ffin_w, ffout_w)
    lane = lax.broadcasted_iota(jnp.int32, (1, 128), 1)
    scalars = jnp.zeros((1, 128), F32)
    msg[...] = jnp.zeros((32, 8, 128), F32)
    for m in range(6):
        units = [u for u in range(N_UNITS) if UNITS[u][0] == m]
        n_loc, n_col = LOC_ROWS[m], N_COLS[m]
        col_s = [0.0] * (n_col // 512)
        col_d = [0.0] * (n_col // 512)
        new_rows = []
        total = jnp.zeros((1, 1), F32)
        for h in range(n_loc // 16):
            here = [u for u in units if UNITS[u][1] == 16 * h]
            squares = {u: gsum[u] * gsum[u] for u in here}
            row_sum = sum(jnp.sum(squares[u] + EPS_SQUARE, axis=1, keepdims=True) for u in here)
            old = rows_in[m][m, :] if m < 4 else rows_in[m][0, :]
            pick = lax.broadcasted_iota(jnp.int32, (16, n_loc), 0) + 16 * h == lax.broadcasted_iota(
                jnp.int32, (16, n_loc), 1)
            old_col = jnp.sum(jnp.where(pick, jnp.broadcast_to(old.reshape(1, n_loc), (16, n_loc)), 0.0),
                              axis=1, keepdims=True)
            new = BETA_TWO * old_col + KEEP * (row_sum / n_col)
            row_out[pl.ds(ROW_AT[m] + 16 * h, 16), :] = jnp.broadcast_to(new, (16, 128))
            total = total + jnp.sum(new, axis=0, keepdims=True)
            new_rows.append((new, here, squares))
        mean = total / n_loc
        for new, here, squares in new_rows:
            inv = mean / new
            for u in here:
                c = UNITS[u][2] // 512
                col_s[c] = col_s[c] + jnp.sum(squares[u] + EPS_SQUARE, axis=0, keepdims=True)
                col_d[c] = col_d[c] + jnp.sum(squares[u] * inv, axis=0, keepdims=True)
        for g in range(n_col // 128):
            at = GROUP_AT[m] + g
            part = slice(128 * (g % 4), 128 * (g % 4) + 128)
            row = 0 if at < 32 else 2
            msg[at % 32, row:row + 1, :] = col_s[g // 4][:, part]
            msg[at % 32, row + 1:row + 2, :] = col_d[g // 4][:, part]
        w = weights[m][m] if m < 4 else weights[m][...]
        w_sq = sum_all(w * w)
        scalars = scalars + jnp.where(lane == m, total, 0.0) + jnp.where(lane == 8 + m, w_sq, 0.0)

    @pl.loop(0, 32)
    def _(p):
        msg[p, 4:5, :] = scalars

    def exchange(k, src_of, dst):
        sends = []
        for t in range(1, 32):
            to = (me + t) % 32
            sends.append(pltpu.make_async_remote_copy(
                src_ref=src_of(to), dst_ref=dst.at[me], send_sem=x_sem.at[2 * k], recv_sem=x_sem.at[2 * k + 1],
                device_id=(to,), device_id_type=MESH))
        for send in sends:
            send.start()

    def all_in(k, dst):
        some = dst.at[pl.ds(0, 31)]
        pltpu.make_async_copy(some, some, x_sem.at[2 * k + 1]).wait()

    def all_out(k, dst):
        some = dst.at[pl.ds(0, 31)]
        pltpu.make_async_copy(some, some, x_sem.at[2 * k]).wait()

    exchange(0, lambda to: msg.at[to], rx)
    rx[me] = msg[me]
    all_in(0, rx)

    scal = rx[:, 4, :]
    mat0, mat1 = me // 8, 4 + me // 4
    n_loc1 = jnp.where(me < 4, 32.0, 16.0)
    n_row1 = jnp.where(me < 4, 1024.0, 512.0)
    lanes = lax.broadcasted_iota(jnp.int32, (32, 128), 1)

    def group(row, mat, n_row):
        sums = jnp.sum(jnp.where(lanes == mat, scal, 0.0), axis=1, keepdims=True)
        ratio = jnp.sum(sums, axis=0, keepdims=True) / 32.0 / sums
        s_sum = jnp.sum(rx[:, row, :], axis=0, keepdims=True)
        d_sum = jnp.sum(rx[:, row + 1, :] * ratio, axis=0, keepdims=True)
        at = me + 32 * (row // 2)
        new = BETA_TWO * col_in[pl.ds(at, 1), :] + KEEP * (s_sum / n_row)
        part = jnp.sum(d_sum / new, axis=1, keepdims=True)
        return new, jnp.broadcast_to(part, (1, 128))

    new0, part0 = group(0, mat0, 1024.0)
    new1, part1 = group(2, jnp.minimum(mat1, 5), n_row1)
    tile[...] = jnp.zeros((8, 128), F32)
    tile[0:1, :] = new0
    tile[1:2, :] = new1
    tile[2:3, :] = part0
    tile[3:4, :] = part1
    exchange(1, lambda to: tile, rb)
    rb[me] = tile[...]
    stat_out[pl.ds(32, 1), 0:1, :] = jnp.sum(scal, axis=0, keepdims=True).reshape(1, 1, 128)
    all_in(1, rb)

    @pl.loop(0, 32)
    def _(p):
        stat_out[p] = rb[p]

    all_out(0, msg)
    all_out(1, rb)
    for u in range(N_UNITS):
        for s in range(5):
            copy(u, s).wait_send()


def dense_sums(attn_g, ffin_g, ffout_g, attn_w, ffin_w, ffout_w, attn_r, ffin_r, ffout_r, col_in):
    vmem = pl.BlockSpec(memory_space=pltpu.VMEM)
    hbm = pl.BlockSpec(memory_space=pl.ANY)
    block = (BLK_R, BLK_C)
    return pl.pallas_call(
        dense_kernel,
        out_shape=(jax.ShapeDtypeStruct((N_UNITS,) + block, F32), jax.ShapeDtypeStruct((176, 128), F32),
                   jax.ShapeDtypeStruct((33, 8, 128), F32)),
        in_specs=[hbm] * 3 + [vmem] * 7,
        out_specs=(vmem,) * 3,
        scratch_shapes=[
            pltpu.VMEM((N_UNITS, 32) + block, jnp.bfloat16),
            pltpu.VMEM((N_UNITS, 16) + block, F32),
            pltpu.VMEM((N_UNITS, 16) + block, F32),
            pltpu.VMEM((N_UNITS, 8) + block, F32),
            pltpu.VMEM((N_UNITS, 4) + block, F32),
            pltpu.VMEM((N_UNITS, 2) + block, F32),
            pltpu.VMEM((N_UNITS, 1) + block, F32),
            pltpu.VMEM((32, 8, 128), F32),
            pltpu.VMEM((32, 8, 128), F32),
            pltpu.VMEM((8, 128), F32),
            pltpu.VMEM((32, 8, 128), F32),
            pltpu.SemaphoreType.DMA((N_UNITS,)),
            pltpu.SemaphoreType.DMA((5, N_UNITS)),
            pltpu.SemaphoreType.DMA((5, N_UNITS)),
            pltpu.SemaphoreType.DMA((4,)),
        ],
        compiler_params=pltpu.CompilerParams(has_side_effects=True, vmem_limit_bytes=56 * 2 ** 20),
        name="dense_sums",
    )(attn_g, ffin_g, ffout_g, attn_w, ffin_w, ffout_w, attn_r, ffin_r, ffout_r, col_in)


def factored_step(gradient, weight, row_state, col_state):
    n_rows = gradient.shape[-2]
    n_elems = n_rows * gradient.shape[-1]
    square = gradient * gradient + EPS_SQUARE
    row_new = BETA_TWO * row_state + KEEP * jnp.mean(square, axis=-1)
    col_new = BETA_TWO * col_state + KEEP * (jnp.sum(square, axis=-2) / n_rows)
    row_mean = jnp.sum(row_new, axis=-1) / n_rows
    row_factor = lax.rsqrt(row_new / row_mean[..., None])
    update = gradient * row_factor[..., :, None] * lax.rsqrt(col_new)[..., None, :]
    upd_rms = jnp.sqrt(jnp.sum(update * update, axis=(-2, -1)) / n_elems)
    w_rms = jnp.sqrt(jnp.sum(weight * weight, axis=(-2, -1)) / n_elems)
    step_coeff = LEARN_RATE * jnp.maximum(EPS_SCALE, w_rms) / jnp.maximum(1.0, upd_rms)
    return weight - step_coeff[..., None, None] * update, row_new, col_new


def solution(mesh):
    dense_specs = (
        (P("dp"), P(None, "dp", None), P(None, "dp"), P()),
        (P("dp"), P("dp", None), P("dp"), P()),
        (P("dp"), P("dp", None), P("dp"), P()),
    )
    expert_specs = ((P("dp"), P("dp"), P("dp"), P("dp")),) * 2
    all_specs = dense_specs + expert_specs
    in_specs = tuple(part_spec for group in all_specs for part_spec in group)
    out_specs = tuple(part_spec for group in all_specs for part_spec in group[1:])

    def update_all(*arrays):
        (ag, aw, ar, ac, ig, iw, ir, ic, og, ow, orow, oc) = arrays[:12]
        col_in = jnp.concatenate([ac.reshape(-1, 128), ic.reshape(-1, 128), oc.reshape(-1, 128),
                                  jnp.ones((20, 128), F32)])
        gsum, rows, stat = dense_sums(
            ag.reshape(4, 32, 32, 1024), ig.reshape(32, 32, 512), og.reshape(32, 16, 1024), aw, iw, ow,
            ar, ir.reshape(1, 32), orow.reshape(1, 16), col_in)
        results = []
        scal = stat[32, 0]
        for m in range(6):
            n_row, n_col, n_loc = N_ROWS[m], N_COLS[m], LOC_ROWS[m]
            here = [u for u in range(N_UNITS) if UNITS[u][0] == m]
            g = jnp.concatenate([jnp.concatenate([gsum[u] for u in here if UNITS[u][1] == 16 * h], axis=1)
                                 for h in range(n_loc // 16)], axis=0)
            w = aw[m] if m < 4 else (iw, ow)[m - 4]
            r_new = rows[ROW_AT[m]:ROW_AT[m] + n_loc, 0]
            if m < 4:
                c_new = stat[8 * m:8 * m + 8, 0].reshape(-1)
                part = jnp.sum(stat[8 * m:8 * m + 8, 2, 0])
            elif m == 4:
                c_new = stat[0:4, 1].reshape(-1)
                part = jnp.sum(stat[0:4, 3, 0])
            else:
                c_new = stat[4:12, 1].reshape(-1)
                part = jnp.sum(stat[4:12, 3, 0])
            n_elems = n_row * n_col
            factor = lax.rsqrt(r_new / (scal[m] / n_row))
            upd_rms = jnp.sqrt(part / n_elems)
            w_rms = jnp.sqrt(scal[8 + m] / n_elems)
            coeff = LEARN_RATE * jnp.maximum(EPS_SCALE, w_rms) / jnp.maximum(1.0, upd_rms)
            results.append((w - coeff * (g * factor[:, None] * lax.rsqrt(c_new)[None, :]), r_new, c_new))
        out = [jnp.stack([results[m][k] for m in range(4)]) for k in range(3)]
        out += list(results[4]) + list(results[5])
        for index in (3, 4):
            out.extend(factored_step(*arrays[4 * index: 4 * index + 4]))
        return tuple(out)

    return jax.shard_map(update_all, mesh=mesh, in_specs=in_specs, out_specs=out_specs, check_vma=False)
```

```python
import functools

import jax
import jax.numpy as jnp
from jax import lax
from jax.experimental import pallas as pl
from jax.experimental.pallas import tpu as pltpu
from jax.sharding import PartitionSpec as P

D_MODEL, D_FF, LANES, N_DEV = 1024, 512, 128, 32
OPT_STEP = 10
LEARN_RATE = 0.1
EPS_SQUARE = 1e-30
EPS_SCALE = 1e-3
BETA_TWO = 1.0 - OPT_STEP ** -0.8
KEEP = 1.0 - BETA_TWO
F32 = jnp.float32
BLK_R, BLK_C = 16, D_FF
N_UNITS = 20
BIT = {"x": 1, "y": 2, "a": 3, "b": 4}

ORDERS = ("xayb", "yaxb") * 10
STEP_UNITS = "".join((
    "ABCADBEFGHIJCKDLMANOPQBERFSTCDBAGCEHFADBIEGAJCBHFDCKGILEDJHF",
    "EMIKNGFLJHGOKMPIHNLJIQMORKJPNLKMSOQTLMRPNOQSNROTPQSRPTQSRTST",
))
STEPS = [(ord(u) - ord("A"), STEP_UNITS[:n].count(u)) for n, u in enumerate(STEP_UNITS)]

UNITS = [(m, 16 * r, D_FF * c) for m in range(4) for r in range(2) for c in range(2)]
UNITS += [(4, 0, 0), (4, 16, 0), (5, 0, 0), (5, 0, D_FF)]
N_ROWS = (D_MODEL, D_MODEL, D_MODEL, D_MODEL, D_MODEL, D_FF)
N_COLS = (D_MODEL, D_MODEL, D_MODEL, D_MODEL, D_FF, D_MODEL)
LOC_ROWS = (N_DEV, N_DEV, N_DEV, N_DEV, N_DEV, 16)
ROW_AT = (0, N_DEV, 64, 96, LANES, 160)
GROUP_AT = (0, 8, 16, 24, N_DEV, 36)
EARLY = 4
WORK_AT, WORK_EVERY = 16, 3
MESH = pl.DeviceIdType.MESH


def sum_of(value, axis):
    return jnp.sum(value, axis=axis, keepdims=True)


over_rows, over_cols = (functools.partial(sum_of, axis=axis) for axis in range(2))


def sum_all(value):
    return over_rows(over_cols(value))


def step_size(upd_sq, w_sq, n_elems):
    w_rms = jnp.sqrt(w_sq / n_elems)
    return LEARN_RATE * jnp.maximum(EPS_SCALE, w_rms) / jnp.maximum(1.0, jnp.sqrt(upd_sq / n_elems))


def expert_work(loads, arrays, results, sums, factor, acc, out_sem, outs):
    g_v, w_v = arrays[0].at[0], arrays[1].at[0]
    r_old, c_old = arrays[2:]
    w_new, r_new, c_new = results
    n_rows, n_cols = g_v.shape
    c_acc, w_acc, u_acc = (acc.at[n, :, pl.ds(0, n_cols)] for n in range(3))
    quarter = n_rows // 4

    def begin():
        for load in loads:
            load.wait()
        for ref in (c_acc, w_acc, u_acc):
            ref[...] = jnp.zeros((8, n_cols), F32)

    def squares(b):
        c_sum, w_sum = c_acc[...], w_acc[...]
        for r in range(16):
            at = slice(LANES * b + 8 * r, LANES * b + 8 * r + 8)
            sq = g_v[at, :] * g_v[at, :] + EPS_SQUARE
            c_sum = c_sum + sq
            w_sum = w_sum + w_v[at, :] * w_v[at, :]
            sums[8 * r:8 * r + 8, :] = jnp.broadcast_to(over_cols(sq), (8, LANES))
        c_acc[...], w_acc[...] = c_sum, w_sum
        part = slice(LANES * b, LANES * b + LANES)
        r_new[:, part] = BETA_TWO * r_old[:, part] + KEEP * (jnp.transpose(sums[...])[0:1, :] / n_cols)

    def factors():
        c_new[...] = BETA_TWO * c_old[...] + KEEP * (over_rows(c_acc[...]) / n_rows)
        mean = over_cols(r_new[...]) / n_rows
        row_factor = lax.rsqrt(r_new[...] / mean)
        for b in range(n_rows // LANES):
            part = slice(LANES * b, LANES * b + LANES)
            factor[part, :] = jnp.transpose(jnp.broadcast_to(row_factor[:, part], (LANES, LANES)))

    def update(q):
        col_factor = lax.rsqrt(c_new[...])

        @pl.loop(0, quarter // N_DEV)
        def _(n):
            at = pl.ds(q * quarter + n * N_DEV, N_DEV)
            upd = g_v[at, :] * factor[at, 0:1] * col_factor
            g_v[at, :] = upd
            sq = upd * upd
            u_acc[...] = u_acc[...] + sq[0:8] + sq[8:16] + sq[16:24] + sq[24:N_DEV]

    def finish(q):
        coeff = step_size(sum_all(u_acc[...]), sum_all(w_acc[...]), n_rows * n_cols)

        @pl.loop(0, quarter // N_DEV)
        def _(n):
            at = pl.ds(q * quarter + n * N_DEV, N_DEV)
            w_v[at, :] = w_v[at, :] - coeff * g_v[at, :]

        part = pl.ds(q * quarter, quarter)
        outs.append(pltpu.make_async_copy(w_v.at[part], w_new.at[part], out_sem(q)))
        outs[-1].start()

    pieces = [begin] + [functools.partial(squares, b) for b in range(n_rows // LANES)] + [factors]
    return pieces + [functools.partial(f, q) for f in (update, finish) for q in range(4)]


def dense_kernel(attn_g, ffin_g, ffout_g, *refs):
    small, expert_in, refs = refs[:9], refs[9:17], refs[17:]
    (gsum, row_out, stat_out), expert_out, scratch = refs[:3], refs[3:9], refs[9:]
    small_vmem, expert_v, scratch = scratch[:9], scratch[9:17], scratch[17:]
    raw, stage, r0, r1, r2, r3, r4, msg, rx, tile, rb, *scratch = scratch
    sums, factor, acc, ld_sem, s_sem, r_sem, x_sem, e_sem = scratch
    attn_w, ffin_w, ffout_w, attn_r, ffin_r, ffout_r, attn_c, ffin_c, ffout_c = small_vmem
    me = lax.axis_index("dp")
    bits = [(me // 2 ** k) % 2 for k in range(5)]
    partner = [me + (1 - 2 * bits[k]) * 2 ** k for k in range(5)]
    core = bits[0]
    recvs = (r0, r1, r2, r3, r4)

    def source(u):
        m, row, col = UNITS[u]
        if m < 4:
            return attn_g.at[m, :, pl.ds(row, BLK_R), pl.ds(col, BLK_C)]
        ref = ffin_g if m == 4 else ffout_g
        return ref.at[:, pl.ds(row, BLK_R), pl.ds(col, BLK_C)]

    barrier = pltpu.get_barrier_semaphore()
    for t in range(1, N_DEV):
        pl.semaphore_signal(barrier, inc=1, device_id=((me + t) % N_DEV,), device_id_type=MESH)
    loads = [pltpu.make_async_copy(source(u), raw.at[u], ld_sem.at[u]) for u in range(N_UNITS)]
    for load in loads:
        load.start()
    small_loads = [pltpu.make_async_copy(a, b, ld_sem.at[N_UNITS]) for a, b in zip(small, small_vmem)]
    for load in small_loads:
        load.start()

    def dest(order, i):
        return sum(((i // 2 ** (3 - j)) % 2) * 2 ** BIT[order[j]] for j in range(4))

    def copy(u, s):
        order = ORDERS[u]
        if s == 0:
            src, to = stage.at[u], partner[0]
        else:
            keep = sum(bits[BIT[order[j]]] * 2 ** (3 - j) for j in range(s - 1))
            k = BIT[order[s - 1]]
            src = r0.at[u, pl.ds(keep + (1 - bits[k]) * 2 ** (4 - s), 2 ** (4 - s))]
            to = partner[k]
        return pltpu.make_async_remote_copy(
            src_ref=src, dst_ref=recvs[s].at[u], send_sem=s_sem.at[s, u], recv_sem=r_sem.at[s, u],
            device_id=(to,), device_id_type=MESH)

    def block_sum(u, s, i, d):
        total = raw[u, d].astype(F32)
        for j in range(s):
            total = total + recvs[j][u, i % 2 ** (4 - j)]
        return total

    def to_f32(u):
        loads[u].wait()

        @pl.loop(0, 16)
        def _(i):
            stage[u, i] = raw[u, dest(ORDERS[u], i) + 1 - core].astype(F32)

    def step(u, s):
        order = ORDERS[u]
        if s == 0:
            to_f32(u)
        else:
            copy(u, s - 1).wait_recv()
            base = sum(bits[BIT[order[j]]] * 2 ** (3 - j) for j in range(min(s - 1, 4)))
            if s == 5:
                gsum[u] = block_sum(u, 5, base, me) * (1.0 / 32.0)
                return
            base = base + (1 - bits[BIT[order[s - 1]]]) * 2 ** (4 - s)

            @pl.loop(0, 2 ** (4 - s))
            def _(n):
                i = base + n
                r0[u, i] = block_sum(u, s, i, dest(order, i) + core)
        copy(u, s).start()

    stage_zero = [u for u, s in STEPS if s == 0]
    for u in stage_zero[:EARLY]:
        to_f32(u)
    pl.semaphore_wait(barrier, 31)
    for u in stage_zero[:EARLY]:
        copy(u, 0).start()
    expert_loads = [pltpu.make_async_copy(a, b, e_sem.at[n]) for n, (a, b) in enumerate(zip(expert_in, expert_v))]
    work = []
    outs = []
    for k in range(2):
        half = slice(4 * k, 4 * k + 4)
        work += expert_work(expert_loads[half], expert_v[half], expert_out[3 * k:3 * k + 3], sums, factor,
                            acc.at[k], lambda n, k=k: e_sem.at[8 + 4 * k + n], outs)
    for n, (u, s) in enumerate(STEPS):
        if n == WORK_AT - 4:
            for load in expert_loads:
                load.start()
        if s > 0 or u not in stage_zero[:EARLY]:
            step(u, s)
        if n >= WORK_AT and n % WORK_EVERY == 0 and work:
            work.pop(0)()
    for piece in work:
        piece()

    for load in small_loads:
        load.wait()

    rows_in = (attn_r, attn_r, attn_r, attn_r, ffin_r, ffout_r)
    weights = (attn_w, attn_w, attn_w, attn_w, ffin_w, ffout_w)
    lane = lax.broadcasted_iota(jnp.int32, (1, LANES), 1)
    scalars = jnp.zeros((1, LANES), F32)
    msg[...] = jnp.zeros((N_DEV, 8, LANES), F32)
    for m in range(6):
        units = [u for u in range(N_UNITS) if UNITS[u][0] == m]
        n_loc, n_col = LOC_ROWS[m], N_COLS[m]
        col_s = [0.0] * (n_col // D_FF)
        col_d = [0.0] * (n_col // D_FF)
        new_rows = []
        total = jnp.zeros((1, 1), F32)
        for h in range(n_loc // 16):
            here = [u for u in units if UNITS[u][1] == 16 * h]
            squares = {u: gsum[u] * gsum[u] for u in here}
            row_sum = sum(over_cols(squares[u] + EPS_SQUARE) for u in here)
            old = rows_in[m][m, :] if m < 4 else rows_in[m][0, :]
            pick = lax.broadcasted_iota(jnp.int32, (16, n_loc), 0) + 16 * h == lax.broadcasted_iota(
                jnp.int32, (16, n_loc), 1)
            old_col = over_cols(jnp.where(pick, jnp.broadcast_to(old.reshape(1, n_loc), (16, n_loc)), 0.0))
            new = BETA_TWO * old_col + KEEP * (row_sum / n_col)
            row_out[pl.ds(ROW_AT[m] + 16 * h, 16), :] = jnp.broadcast_to(new, (16, LANES))
            total = total + over_rows(new)
            new_rows.append((new, here, squares))
        mean = total / n_loc
        for new, here, squares in new_rows:
            inv = mean / new
            for u in here:
                c = UNITS[u][2] // D_FF
                col_s[c] = col_s[c] + over_rows(squares[u] + EPS_SQUARE)
                col_d[c] = col_d[c] + over_rows(squares[u] * inv)
        for g in range(n_col // LANES):
            at = GROUP_AT[m] + g
            part = slice(LANES * (g % 4), LANES * (g % 4) + LANES)
            row = 0 if at < N_DEV else 2
            msg[at % N_DEV, row:row + 1, :] = col_s[g // 4][:, part]
            msg[at % N_DEV, row + 1:row + 2, :] = col_d[g // 4][:, part]
        w = weights[m][m] if m < 4 else weights[m][...]
        w_sq = sum_all(w * w)
        scalars = scalars + jnp.where(lane == m, total, 0.0) + jnp.where(lane == 8 + m, w_sq, 0.0)

    @pl.loop(0, N_DEV)
    def _(p):
        msg[p, 4:5, :] = scalars

    def exchange(k, src_of, dst):
        sends = []
        for t in range(1, N_DEV):
            to = (me + t) % N_DEV
            sends.append(pltpu.make_async_remote_copy(
                src_ref=src_of(to), dst_ref=dst.at[me], send_sem=x_sem.at[2 * k], recv_sem=x_sem.at[2 * k + 1],
                device_id=(to,), device_id_type=MESH))
        for send in sends:
            send.start()

    def all_in(k, dst):
        some = dst.at[pl.ds(0, 31)]
        pltpu.make_async_copy(some, some, x_sem.at[2 * k + 1]).wait()

    def all_out(k, dst):
        some = dst.at[pl.ds(0, 31)]
        pltpu.make_async_copy(some, some, x_sem.at[2 * k]).wait()

    exchange(0, lambda to: msg.at[to], rx)
    rx[me] = msg[me]
    all_in(0, rx)

    scal = rx[:, 4, :]
    mat0, mat1 = me // 8, 4 + me // 4
    n_loc1 = jnp.where(me < 4, 32.0, 16.0)
    n_row1 = jnp.where(me < 4, 1024.0, 512.0)
    lanes = lax.broadcasted_iota(jnp.int32, (N_DEV, LANES), 1)

    def group(row, mat, n_row, old):
        sums = over_cols(jnp.where(lanes == mat, scal, 0.0))
        ratio = over_rows(sums) / 32.0 / sums
        s_sum = over_rows(rx[:, row, :])
        d_sum = over_rows(rx[:, row + 1, :] * ratio)
        new = BETA_TWO * old + KEEP * (s_sum / n_row)
        part = over_cols(d_sum / new)
        return new, jnp.broadcast_to(part, (1, LANES))

    def lanes_at(k):
        return pl.ds(pl.multiple_of(k * LANES, LANES), LANES)

    old0 = sum(jnp.where(mat0 == m, attn_c[m:m + 1, lanes_at(me % 8)], 0.0) for m in range(4))
    old1 = jnp.where(me < 4, ffin_c[:, lanes_at(me % 4)], ffout_c[:, lanes_at((me + 4) % 8)])
    new0, part0 = group(0, mat0, 1024.0, old0)
    new1, part1 = group(2, jnp.minimum(mat1, 5), n_row1, old1)
    tile[...] = jnp.zeros((8, LANES), F32)
    tile[0:1, :] = new0
    tile[1:2, :] = new1
    tile[2:3, :] = part0
    tile[3:4, :] = part1
    exchange(1, lambda to: tile, rb)
    rb[me] = tile[...]
    stat_out[pl.ds(N_DEV, 1), 0:1, :] = over_rows(scal).reshape(1, 1, LANES)
    all_in(1, rb)

    @pl.loop(0, N_DEV)
    def _(p):
        stat_out[p] = rb[p]

    for out in outs:
        out.wait()
    all_out(0, msg)
    all_out(1, rb)
    for u in range(N_UNITS):
        for s in range(5):
            copy(u, s).wait_send()


ANY = pl.BlockSpec(memory_space=pl.ANY)
VMEM = pl.BlockSpec(memory_space=pltpu.VMEM)


EXPERT_SHAPES = ((D_MODEL, D_FF), (1, D_MODEL), (1, D_FF), (D_FF, D_MODEL), (1, D_FF), (1, D_MODEL))


def shapes_of(*shapes):
    return tuple(jax.ShapeDtypeStruct(shape, F32) for shape in shapes)


def dense_sums(grads, small, experts):
    block = (BLK_R, BLK_C)
    halves = [pltpu.VMEM((N_UNITS, 2 ** k) + block, F32) for k in (4, 4, 3, 2, 1, 0)]
    return pl.pallas_call(
        dense_kernel,
        out_shape=shapes_of((N_UNITS,) + block, (176, LANES), (33, 8, LANES), *EXPERT_SHAPES),
        in_specs=[ANY] * 20,
        out_specs=(VMEM,) * 3 + (ANY, VMEM, VMEM) * 2,
        scratch_shapes=[pltpu.VMEM(a.shape, F32) for a in small + experts] + [
            pltpu.VMEM((N_UNITS, N_DEV) + block, jnp.bfloat16), *halves,
            pltpu.VMEM((N_DEV, 8, LANES), F32), pltpu.VMEM((N_DEV, 8, LANES), F32),
            pltpu.VMEM((8, LANES), F32), pltpu.VMEM((N_DEV, 8, LANES), F32),
            pltpu.VMEM((LANES, LANES), F32), pltpu.VMEM((D_MODEL, LANES), F32), pltpu.VMEM((2, 3, 8, D_MODEL), F32),
            pltpu.SemaphoreType.DMA((N_UNITS + 1,)),
            pltpu.SemaphoreType.DMA((5, N_UNITS)),
            pltpu.SemaphoreType.DMA((5, N_UNITS)),
            pltpu.SemaphoreType.DMA((4,)),
            pltpu.SemaphoreType.DMA((16,)),
        ],
        compiler_params=pltpu.CompilerParams(
            has_side_effects=True, vmem_limit_bytes=58 * 2 ** 20, collective_id=1),
        name="dense_sums",
    )(*grads, *small, *experts)


def final_kernel(gsum, rows, stat, *refs):
    dense_w, expert_in, refs = refs[:3], refs[3:9], refs[9:]
    (aw_new, ar_new, ac_new, iw_new, ir_new, ic_new, ow_new, or_new, oc_new), refs = refs[:9], refs[9:]
    expert_out, (gs_v, aw, iw, ow, e_in, e_out, in_sem, out_sem) = refs[:6], refs[6:]

    dense_loads = [pltpu.make_async_copy(a, b, in_sem.at[n])
                   for n, (a, b) in enumerate(zip((gsum,) + dense_w, (gs_v, aw, iw, ow)))]
    moves = []
    for k, buffer in enumerate((e_in, e_out)):
        n_rows = buffer.shape[0] // 4
        for q in range(4):
            part = pl.ds(q * n_rows, n_rows)
            moves.append((pltpu.make_async_copy(expert_in[3 * k].at[part], buffer.at[part], in_sem.at[4 + 4 * k + q]),
                          pltpu.make_async_copy(buffer.at[part], expert_out[3 * k].at[0, part],
                                                out_sem.at[3 + 4 * k + q])))
    for load in dense_loads:
        load.start()
    for load, _ in moves:
        load.start()
    for k in (1, 2, 4, 5):
        expert_out[k][...] = expert_in[k][...]
    for load in dense_loads:
        load.wait()

    scal = stat[N_DEV, 0:1, :]
    lane = lax.broadcasted_iota(jnp.int32, (1, LANES), 1)
    flipped = (jnp.transpose(rows[0:LANES, :]), jnp.transpose(rows[48:176, :]))
    for m in range(4):
        ar_new[m:m + 1, :] = flipped[0][0:1, N_DEV * m:N_DEV * m + N_DEV]
    ir_new[...] = flipped[1][0:1, 80:112]
    or_new[...] = flipped[1][0:1, 112:LANES]
    outs = []
    for m in range(6):
        row = 0 if m < 4 else 1
        at = GROUP_AT[m] % N_DEV
        n_groups = N_COLS[m] // LANES
        c_new = jnp.concatenate([stat[at + g, row:row + 1, :] for g in range(n_groups)], axis=1)
        parts = sum(stat[at + g, row + 2:row + 3, 0:1] for g in range(n_groups))
        if m < 4:
            ac_new[m:m + 1, :] = c_new
        else:
            (ic_new, oc_new)[m - 4][...] = c_new
        row_total = over_cols(jnp.where(lane == m, scal, 0.0))
        w_sq = over_cols(jnp.where(lane == 8 + m, scal, 0.0))
        coeff = step_size(parts, w_sq, N_ROWS[m] * N_COLS[m])
        col_factor = lax.rsqrt(c_new)
        w = aw.at[m] if m < 4 else (iw, ow)[m - 4]
        for u in range(N_UNITS):
            if UNITS[u][0] != m:
                continue
            r_at, c_at = UNITS[u][1:]
            r_factor = lax.rsqrt(rows[ROW_AT[m] + r_at:ROW_AT[m] + r_at + BLK_R, 0:1] / (row_total / N_ROWS[m]))
            step = coeff * (gs_v[u] * r_factor * col_factor[:, c_at:c_at + BLK_C])
            part = (slice(r_at, r_at + BLK_R), slice(c_at, c_at + BLK_C))
            w[part] = w[part] - step
        if m >= 3:
            outs.append(pltpu.make_async_copy((aw, iw, ow)[m - 3], (aw_new, iw_new, ow_new)[m - 3],
                                              out_sem.at[m - 3]))
            outs[-1].start()
    for load, out in moves:
        load.wait()
        out.start()
        outs.append(out)
    for out in outs:
        out.wait()


def final_update(sums, dense_w):
    experts = [(1,) + shape if shape[0] > 1 else shape for shape in EXPERT_SHAPES]
    return pl.pallas_call(
        final_kernel,
        out_shape=shapes_of((4, N_DEV, D_MODEL), (4, N_DEV), (4, D_MODEL), (N_DEV, D_FF), (1, N_DEV), (1, D_FF), (16, D_MODEL), (1, 16),
                            (1, D_MODEL), *experts),
        in_specs=[ANY, VMEM, VMEM] + [ANY] * 3 + [ANY, VMEM, VMEM] * 2,
        out_specs=[ANY, VMEM, VMEM] * 5,
        scratch_shapes=[
            pltpu.VMEM((N_UNITS, BLK_R, BLK_C), F32), *[pltpu.VMEM(a.shape, F32) for a in dense_w],
            pltpu.VMEM((D_MODEL, D_FF), F32), pltpu.VMEM((D_FF, D_MODEL), F32),
            pltpu.SemaphoreType.DMA((12,)), pltpu.SemaphoreType.DMA((11,)),
        ],
        compiler_params=pltpu.CompilerParams(vmem_limit_bytes=67043328),
        name="final_update",
    )(*sums[:3], *dense_w, *sums[3:])


def solution(mesh):
    dense_specs = (
        (P("dp"), P(None, "dp", None), P(None, "dp"), P()),
        (P("dp"), P("dp", None), P("dp"), P()),
        (P("dp"), P("dp", None), P("dp"), P()),
    )
    expert_specs = ((P("dp"), P("dp"), P("dp"), P("dp")),) * 2
    all_specs = dense_specs + expert_specs
    in_specs = tuple(part_spec for group in all_specs for part_spec in group)
    out_specs = tuple(part_spec for group in all_specs for part_spec in group[1:])

    def update_all(*arrays):
        (ag, aw, ar, ac, ig, iw, ir, ic, og, ow, orow, oc) = arrays[:12]
        grads = (ag.reshape(4, N_DEV, N_DEV, D_MODEL), ig.reshape(N_DEV, N_DEV, D_FF), og.reshape(N_DEV, 16, D_MODEL))
        sums = dense_sums(grads, (aw, iw, ow, ar, ir.reshape(1, N_DEV), orow.reshape(1, 16),
                                  ac, ic.reshape(1, D_FF), oc.reshape(1, D_MODEL)), arrays[12:])
        out = final_update(sums, (aw, iw, ow))
        return tuple(o.reshape(-1) if n in (4, 5, 7, 8) else o for n, o in enumerate(out))

    return jax.shard_map(update_all, mesh=mesh, in_specs=in_specs, out_specs=out_specs, check_vma=False)
```

```python
import functools

import jax
import jax.numpy as jnp
from jax import lax
from jax.experimental import pallas as pl
from jax.experimental.pallas import tpu as pltpu
from jax.sharding import PartitionSpec as P

D_MODEL, D_FF, LANES, N_DEV, TILE = 1024, 512, 128, 32, 8
OPT_STEP = 10
LEARN_RATE = 0.1
EPS_SQUARE = 1e-30
EPS_SCALE = 1e-3
BETA_TWO = 1.0 - OPT_STEP ** -0.8
KEEP = 1.0 - BETA_TWO
F32 = jnp.float32
BLK_R, BLK_C = 16, D_FF
N_UNITS = 20
BIT = {"x": 1, "y": 2, "a": 3, "b": 4}

ORDERS = (
    "xayb", "yaxb", "ayxb", "ayxb", "xyab", "axyb", "xyab", "axyb", "xyab", "yxab",
    "yaxb", "yaxb", "xyab", "yxab", "axyb", "yxab", "axyb", "xayb", "yxab", "xyab",
)
STEP_UNITS = "".join((
    "DRFPQDRINGKPINQHRPMCHALGBKCOBQRFGHSAEJTQJBNOMFAICRNHDIBLEPMN",
    "CHRKFDPBGOIKEJQLGDCBOASFMKTIOJLADQMEJTHKLSEAMNCTGFLOJPSETSTS",
))
STEPS = [(ord(u) - ord("A"), STEP_UNITS[:n].count(u)) for n, u in enumerate(STEP_UNITS)]

UNITS = [(m, 16 * r, D_FF * c) for m in range(4) for r in range(2) for c in range(2)]
UNITS += [(5, 0, 0), (5, 0, D_FF), (4, 0, 0), (4, 16, 0)]
N_ROWS = (D_MODEL, D_MODEL, D_MODEL, D_MODEL, D_MODEL, D_FF)
N_COLS = (D_MODEL, D_MODEL, D_MODEL, D_MODEL, D_FF, D_MODEL)
LOC_ROWS = (N_DEV, N_DEV, N_DEV, N_DEV, N_DEV, 16)
ROW_AT = (0, N_DEV, 64, 96, LANES, 160)
LAST = 4
EARLY = 1
WORK_AT, WORK_EVERY = 16, 3
MESH = pl.DeviceIdType.MESH


def sum_of(value, axis):
    return jnp.sum(value, axis=axis, keepdims=True)


over_rows, over_cols = (functools.partial(sum_of, axis=axis) for axis in range(2))


def sum_all(value):
    return over_rows(over_cols(value))


def step_size(upd_sq, w_sq, n_elems):
    w_rms = jnp.sqrt(w_sq / n_elems)
    return LEARN_RATE * jnp.maximum(EPS_SCALE, w_rms) / jnp.maximum(1.0, jnp.sqrt(upd_sq / n_elems))


def expert_work(loads, arrays, results, sums, factor, acc, out_sem, outs):
    g_v, w_v = arrays[0].at[0], arrays[1].at[0]
    r_old, c_old = arrays[2:]
    w_new, r_new, c_new = results
    n_rows, n_cols = g_v.shape
    c_acc, w_acc, u_acc = (acc.at[n, :, pl.ds(0, n_cols)] for n in range(3))
    quarter = n_rows // 4

    def begin():
        for load in loads:
            load.wait()
        for ref in (c_acc, w_acc, u_acc):
            ref[...] = jnp.zeros((TILE, n_cols), F32)

    def squares(b):
        c_sum, w_sum = c_acc[...], w_acc[...]
        for r in range(16):
            at = slice(LANES * b + TILE * r, LANES * b + TILE * r + TILE)
            sq = g_v[at, :] * g_v[at, :] + EPS_SQUARE
            c_sum = c_sum + sq
            w_sum = w_sum + w_v[at, :] * w_v[at, :]
            sums[TILE * r:TILE * r + TILE, :] = jnp.broadcast_to(over_cols(sq), (TILE, LANES))
        c_acc[...], w_acc[...] = c_sum, w_sum
        part = slice(LANES * b, LANES * b + LANES)
        r_new[:, part] = BETA_TWO * r_old[:, part] + KEEP * (jnp.transpose(sums[...])[0:1, :] / n_cols)

    def factors():
        c_new[...] = BETA_TWO * c_old[...] + KEEP * (over_rows(c_acc[...]) / n_rows)
        mean = over_cols(r_new[...]) / n_rows
        row_factor = lax.rsqrt(r_new[...] / mean)
        for b in range(n_rows // LANES):
            part = slice(LANES * b, LANES * b + LANES)
            factor[part, :] = jnp.transpose(jnp.broadcast_to(row_factor[:, part], (LANES, LANES)))

    def update(q):
        col_factor = lax.rsqrt(c_new[...])

        @pl.loop(0, quarter // N_DEV)
        def _(n):
            at = pl.ds(q * quarter + n * N_DEV, N_DEV)
            upd = g_v[at, :] * factor[at, 0:1] * col_factor
            g_v[at, :] = upd
            sq = upd * upd
            u_acc[...] = u_acc[...] + sq[0:TILE] + sq[TILE:16] + sq[16:24] + sq[24:N_DEV]

    def finish(q):
        coeff = step_size(sum_all(u_acc[...]), sum_all(w_acc[...]), n_rows * n_cols)

        @pl.loop(0, quarter // N_DEV)
        def _(n):
            at = pl.ds(q * quarter + n * N_DEV, N_DEV)
            w_v[at, :] = w_v[at, :] - coeff * g_v[at, :]

        part = pl.ds(q * quarter, quarter)
        outs.append(pltpu.make_async_copy(w_v.at[part], w_new.at[part], out_sem(q)))
        outs[-1].start()

    pieces = [begin] + [functools.partial(squares, b) for b in range(n_rows // LANES)] + [factors]
    return pieces + [functools.partial(f, q) for f in (update, finish) for q in range(4)]


def dense_kernel(attn_g, ffin_g, ffout_g, *refs):
    small, expert_in, refs = refs[:9], refs[9:17], refs[17:]
    (gsum, rows_hbm, stat_hbm), expert_hbm, scratch = refs[:3], refs[3:9], list(refs[9:])
    (row_out, stat_out), scratch = scratch[:2], scratch[2:]
    expert_out = [hbm if n % 3 == 0 else scratch.pop(0) for n, hbm in enumerate(expert_hbm)]
    small_vmem, expert_v, scratch = scratch[:9], scratch[9:17], scratch[17:]
    raw, stage, r0, r1, r2, r3, r4, msg, rx, rb, rx_end, rx_row, tile, end, end_row, g_own, rows_msg, rx_rows, *scratch = scratch
    sums, factor, acc, ld_sem, s_sem, r_sem, x_sem, e_sem, o_sem = scratch
    attn_w, ffin_w, ffout_w, attn_r, ffin_r, ffout_r, attn_c, ffin_c, ffout_c = small_vmem
    me = lax.axis_index("dp")
    bits = [(me // 2 ** k) % 2 for k in range(5)]
    partner = [me + (1 - 2 * bits[k]) * 2 ** k for k in range(5)]
    core = bits[0]
    recvs = (r0, r1, r2, r3, r4)

    def source(u):
        m, row, col = UNITS[u]
        if m < 4:
            return attn_g.at[m, :, pl.ds(row, BLK_R), pl.ds(col, BLK_C)]
        ref = ffin_g if m == 4 else ffout_g
        return ref.at[:, pl.ds(row, BLK_R), pl.ds(col, BLK_C)]

    barrier = pltpu.get_barrier_semaphore()
    for t in range(1, N_DEV):
        pl.semaphore_signal(barrier, inc=1, device_id=((me + t) % N_DEV,), device_id_type=MESH)
    loads = [pltpu.make_async_copy(source(u), raw.at[u], ld_sem.at[u]) for u in range(N_UNITS)]
    stage_zero = [u for u, s in STEPS if s == 0]
    for u in stage_zero[:2]:
        loads[u].start()
    small_loads = [pltpu.make_async_copy(a, b, ld_sem.at[N_UNITS]) for a, b in zip(small, small_vmem)]
    def dest(order, i):
        return sum(((i // 2 ** (3 - j)) % 2) * 2 ** BIT[order[j]] for j in range(4))

    def copy(u, s):
        order = ORDERS[u]
        if s == 0:
            src, to = stage.at[u], partner[0]
        else:
            keep = sum(bits[BIT[order[j]]] * 2 ** (3 - j) for j in range(s - 1))
            k = BIT[order[s - 1]]
            src = r0.at[u, pl.ds(keep + (1 - bits[k]) * 2 ** (4 - s), 2 ** (4 - s))]
            to = partner[k]
        return pltpu.make_async_remote_copy(
            src_ref=src, dst_ref=recvs[s].at[u], send_sem=s_sem.at[s], recv_sem=r_sem.at[s, u],
            device_id=(to,), device_id_type=MESH)

    def block_sum(u, s, i, d):
        total = raw[u, d].astype(F32)
        for j in range(s):
            total = total + recvs[j][u, i % 2 ** (4 - j)]
        return total

    rows_in = (attn_r, attn_r, attn_r, attn_r, ffin_r, ffout_r)
    weights = (attn_w, attn_w, attn_w, attn_w, ffin_w, ffout_w)
    lane = lax.broadcasted_iota(jnp.int32, (1, LANES), 1)

    def statistics(m):
        n_loc, n_col = LOC_ROWS[m], N_COLS[m]
        col_s, col_d = ([0.0] * (n_col // D_FF) for _ in range(2))
        new_rows = []
        total = jnp.zeros((1, 1), F32)
        for h in range(n_loc // 16):
            here = [u for u in range(N_UNITS) if UNITS[u][:2] == (m, 16 * h)]
            squares = {u: g_own[u] * g_own[u] for u in here}
            row_sum = sum(over_cols(squares[u] + EPS_SQUARE) for u in here)
            old = rows_in[m][m:m + 1, :] if m < 4 else rows_in[m][...]
            pick = lax.broadcasted_iota(jnp.int32, (16, n_loc), 0) + 16 * h == lax.broadcasted_iota(
                jnp.int32, (16, n_loc), 1)
            old_col = over_cols(jnp.where(pick, jnp.broadcast_to(old, (16, n_loc)), 0.0))
            new = BETA_TWO * old_col + KEEP * (row_sum / n_col)
            row_out[pl.ds(ROW_AT[m] + 16 * h, 16), :] = jnp.broadcast_to(new, (16, LANES))
            total = total + over_rows(new)
            new_rows.append((new, here, squares))
        mean = total / n_loc
        for new, here, squares in new_rows:
            inv = mean / new
            for u in here:
                c = UNITS[u][2] // D_FF
                col_s[c] = col_s[c] + over_rows(squares[u] + EPS_SQUARE)
                col_d[c] = col_d[c] + over_rows(squares[u] * inv)
        return total, col_s, col_d

    z, rest = me // TILE, me % TILE
    z_order = [TILE * (3 - z), TILE * ((z + 2) % 4), TILE * (z + 1 - 2 * (z % 2)), TILE * z]

    def exchange(k, src_of, dst):
        for n, at in enumerate(z_order):
            @pl.loop(n // 3, TILE)
            def _(r, at=at):
                to = at + (rest + r) % TILE
                pltpu.make_async_remote_copy(
                    src_ref=src_of(to), dst_ref=dst.at[me], send_sem=x_sem.at[2 * k], recv_sem=x_sem.at[2 * k + 1],
                    device_id=(to,), device_id_type=MESH).start()

    def wait_all(sem, dst):
        some = dst.at[pl.ds(0, 31)]
        pltpu.make_async_copy(some, some, x_sem.at[sem]).wait()

    def collect_weights():
        rows_msg[...] = sum(jnp.where(lane == TILE + m, sum_all(w * w), 0.0)
                            for m, w in enumerate(weights[m][m] if m < 4 else weights[m][...] for m in range(6)))
        msg[...] = jnp.zeros((N_DEV, 4, LANES), F32)

    def collect(m):
        total, col_s, col_d = statistics(m)
        for g in range(TILE):
            at = TILE * (m % 5) + g
            row = 0 if m < 4 else 2
            part = slice(LANES * (g % 4), LANES * (g % 4) + LANES)
            msg[at, row:row + 1, :] = col_s[g // 4][:, part]
            msg[at, row + 1:row + 2, :] = col_d[g // 4][:, part]
        rows_msg[...] = rows_msg[...] + jnp.where(lane == m, total, 0.0)

    def send_first():
        exchange(0, lambda to: msg.at[to], rx)
        exchange(4, lambda to: rows_msg, rx_rows)
        rx[me] = msg[me]
        rx_rows[me] = rows_msg[...]

    def lanes_at(k):
        return pl.ds(pl.multiple_of(k * LANES, LANES), LANES)

    def own_groups():
        wait_all(1, rx)
        wait_all(9, rx_rows)
        scal = rx_rows[:, 0, :]
        lanes = lax.broadcasted_iota(jnp.int32, (N_DEV, LANES), 1)

        def group(row, mat, n_row, old):
            sums = over_cols(jnp.where(lanes == mat, scal, 0.0))
            ratio = over_rows(sums) / 32.0 / sums
            new = BETA_TWO * old + KEEP * (over_rows(rx[:, row, :]) / n_row)
            part = over_cols(over_rows(rx[:, row + 1, :] * ratio) / new)
            tile[row // 2:row // 2 + 1, :] = new
            tile[row // 2 + 2:row // 2 + 3, :] = jnp.broadcast_to(part, (1, LANES))

        here = lanes_at(me % TILE)
        group(0, me // TILE, 1024.0, sum(jnp.where(me // TILE == m, attn_c[m:m + 1, here], 0.0) for m in range(4)))
        group(2, 5, 512.0, ffout_c[:, here])
        exchange(1, lambda to: tile, rb)
        rb[me] = tile[...]
        stat_out[N_DEV, 0:1, :] = over_rows(scal)

    def send_last():
        total, (col_s,), (col_d,) = statistics(LAST)
        for g in range(4):
            part = slice(LANES * g, LANES * g + LANES)
            end[g:g + 1, :] = col_s[:, part]
            end[g + 4:g + 5, :] = col_d[:, part]
        end_row[...] = jnp.broadcast_to(total, (1, LANES))
        exchange(2, lambda to: end, rx_end)
        exchange(3, lambda to: end_row, rx_row)
        rx_end[me] = end[...]
        rx_row[me] = end_row[...]

    def take_last():
        wait_all(5, rx_end)
        wait_all(7, rx_row)
        rows_all = rx_row[:, 0, :]
        grand = over_rows(rows_all)
        ratio = grand / 32.0 / rows_all
        is_s = lax.broadcasted_iota(jnp.int32, (TILE, LANES), 0) < 4
        both = [jnp.zeros((TILE, LANES), F32) for _ in range(4)]
        for p in range(N_DEV):
            both[p % 4] = both[p % 4] + rx_end[p] * jnp.where(is_s, 1.0, ratio[p:p + 1, :])
        both = (both[0] + both[1]) + (both[2] + both[3])
        col_s, col_d = both[0:4, :], both[4:TILE, :]
        for g in range(4):
            stat_out[33, g:g + 1, :] = ffin_c[:, LANES * g:LANES * g + LANES]
        new = BETA_TWO * stat_out[33, 0:4, :] + KEEP * (col_s / 1024.0)
        stat_out[33, 0:4, :] = new
        stat_out[33, 4:5, :] = jnp.broadcast_to(sum_all(col_d / new), (1, LANES))
        stat_out[33, 5:6, :] = grand

    outs = []

    def put(src, dst, n):
        outs.append(pltpu.make_async_copy(src, dst, o_sem.at[n]))
        outs[-1].start()

    def to_f32(u):
        loads[u].wait()

        @pl.loop(0, 4)
        def _(n):
            for k in range(4):
                i = 4 * n + k
                stage[u, i] = raw[u, dest(ORDERS[u], i) + 1 - core].astype(F32)

    def step(u, s):
        order = ORDERS[u]
        if s == 0:
            to_f32(u)
        else:
            copy(u, s - 1).wait_recv()
            base = sum(bits[BIT[order[j]]] * 2 ** (3 - j) for j in range(min(s - 1, 4)))
            if s == 5:
                g_own[u] = block_sum(u, 5, base, me) * (1.0 / 32.0)
                outs.append(pltpu.make_async_copy(g_own.at[u], gsum.at[u], ld_sem.at[u]))
                outs[-1].start()
                return
            base = base + (1 - bits[BIT[order[s - 1]]]) * 2 ** (4 - s)

            @pl.loop(0, 2 ** (4 - s))
            def _(n):
                i = base + n
                r0[u, i] = block_sum(u, s, i, dest(order, i) + core)
        copy(u, s).start()

    for u in stage_zero[2:TILE]:
        loads[u].start()
    for u in stage_zero[:EARLY]:
        to_f32(u)
    pl.semaphore_wait(barrier, 31)
    for u in stage_zero[:EARLY]:
        copy(u, 0).start()
    for u in stage_zero[TILE:]:
        loads[u].start()
    expert_loads = [pltpu.make_async_copy(a, b, e_sem.at[n]) for n, (a, b) in enumerate(zip(expert_in, expert_v))]
    work = []
    for k in range(2):
        half = slice(4 * k, 4 * k + 4)
        work += expert_work(expert_loads[half], expert_v[half], expert_out[3 * k:3 * k + 3], sums, factor,
                            acc.at[k], lambda n, k=k: e_sem.at[TILE + 4 * k + n], outs)
    left = {m: sum(unit[0] == m for unit in UNITS) for m in range(6)}
    for n, (u, s) in enumerate(STEPS):
        if n == WORK_AT - 4:
            for load in small_loads + expert_loads:
                load.start()
            for load in small_loads:
                load.wait()
            collect_weights()
        if s > 0 or u not in stage_zero[:EARLY]:
            step(u, s)
        if n >= WORK_AT and n % WORK_EVERY == 0 and work:
            work.pop(0)()
        if n == len(STEPS) - TILE:
            for piece in work:
                piece()
        if s == 5:
            m = UNITS[u][0]
            left[m] -= 1
            if left[m] == 0 and m != LAST:
                collect(m)
            if s == 5 and sum(left.values()) == left[LAST] and m != LAST:
                send_first()
    send_last()
    put(row_out, rows_hbm, 0)
    for n in range(6):
        if n % 3:
            put(expert_out[n], expert_hbm[n], n)
    own_groups()

    for k, sent in enumerate((stage, r1, r2, r3, r4)):
        pltpu.make_async_copy(sent, sent, s_sem.at[k]).wait()
    for out in outs:
        out.wait()
    take_last()
    wait_all(3, rb)
    stat_out[pl.ds(0, N_DEV), 0:4, :] = rb[...]
    put(stat_out, stat_hbm, 3)
    outs[-1].wait()
    for k, ref in ((0, msg), (2, rb), (4, rx_end), (6, rx_row), (TILE, rx_rows)):
        wait_all(k, ref)


ANY = pl.BlockSpec(memory_space=pl.ANY)
VMEM = pl.BlockSpec(memory_space=pltpu.VMEM)


EXPERT_SHAPES = ((D_MODEL, D_FF), (1, D_MODEL), (1, D_FF), (D_FF, D_MODEL), (1, D_FF), (1, D_MODEL))


def shapes_of(*shapes):
    return tuple(jax.ShapeDtypeStruct(shape, F32) for shape in shapes)


def dense_sums(grads, small, experts):
    block = (BLK_R, BLK_C)
    vectors = tuple(shape for n, shape in enumerate(EXPERT_SHAPES) if n % 3)
    halves = [pltpu.VMEM((N_UNITS, 2 ** k) + block, F32) for k in (4, 4, 3, 2, 1, 0)]
    return pl.pallas_call(
        dense_kernel,
        out_shape=shapes_of((N_UNITS,) + block, (176, LANES), (34, TILE, LANES), *EXPERT_SHAPES),
        in_specs=[ANY] * 20,
        out_specs=(ANY,) * 9,
        scratch_shapes=[pltpu.VMEM(shape, F32) for shape in ((176, LANES), (34, TILE, LANES)) + vectors] + [
            pltpu.VMEM(a.shape, F32) for a in small + experts] + [
            pltpu.VMEM((N_UNITS, N_DEV) + block, jnp.bfloat16), *halves,
            *[pltpu.VMEM((N_DEV, 4, LANES), F32)] * 3, pltpu.VMEM((N_DEV, TILE, LANES), F32), pltpu.VMEM((N_DEV, 1, LANES), F32),
            pltpu.VMEM((4, LANES), F32), pltpu.VMEM((TILE, LANES), F32), pltpu.VMEM((1, LANES), F32),
            pltpu.VMEM((N_UNITS,) + block, F32), pltpu.VMEM((1, LANES), F32), pltpu.VMEM((N_DEV, 1, LANES), F32),
            pltpu.VMEM((LANES, LANES), F32), pltpu.VMEM((D_MODEL, LANES), F32), pltpu.VMEM((2, 3, TILE, D_MODEL), F32),
            pltpu.SemaphoreType.DMA((N_UNITS + 1,)),
            pltpu.SemaphoreType.DMA((5,)), pltpu.SemaphoreType.DMA((5, N_UNITS)),
            pltpu.SemaphoreType.DMA((10,)),
            pltpu.SemaphoreType.DMA((16,)),
            pltpu.SemaphoreType.DMA((7,)),
        ],
        compiler_params=pltpu.CompilerParams(
            has_side_effects=True, vmem_limit_bytes=58 * 2 ** 20, collective_id=1),
        name="dense_sums",
    )(*grads, *small, *experts)


def final_kernel(gsum, rows_in, stat_in, *refs):
    dense_w, expert_in, refs = refs[:3], refs[3:9], refs[9:]
    (aw_new, ar_new, ac_new, iw_new, ir_new, ic_new, ow_new, or_new, oc_new), refs = refs[:9], refs[9:]
    expert_out, (gs_v, rows, stat, aw, iw, ow, *expert_v), (in_sem, out_sem) = refs[:6], refs[6:-2], refs[-2:]

    dense_loads = [pltpu.make_async_copy(a, b, in_sem.at[n]) for n, (a, b) in enumerate(
        zip((stat_in, rows_in, gsum) + dense_w, (stat, rows, gs_v, aw, iw, ow)))]
    moves = []
    for k in range(6):
        src, via, dst = expert_in[k], expert_v[k], expert_out[k]
        n_parts = 1 if k % 3 else 4
        n_rows = via.shape[0] // n_parts
        for q in range(n_parts):
            part = pl.ds(q * n_rows, n_rows)
            at = len(moves)
            moves.append((pltpu.make_async_copy(src.at[part], via.at[part], in_sem.at[6 + at]),
                          pltpu.make_async_copy(via.at[part], dst.at[part] if n_parts == 1 else dst.at[0, part],
                                                out_sem.at[3 + at])))
    for load in dense_loads:
        load.start()
    for load, _ in moves:
        load.start()
    for load in dense_loads:
        load.wait()

    scal = stat[N_DEV, 0:1, :]
    lane = lax.broadcasted_iota(jnp.int32, (1, LANES), 1)
    flipped = (jnp.transpose(rows[0:LANES, :]), jnp.transpose(rows[48:176, :]))
    for m in range(4):
        ar_new[m:m + 1, :] = flipped[0][0:1, N_DEV * m:N_DEV * m + N_DEV]
    ir_new[...] = flipped[1][0:1, 80:112]
    or_new[...] = flipped[1][0:1, 112:LANES]
    outs = []
    for m in range(6):
        row = m // 5
        row_total = over_cols(jnp.where(lane == m, scal, 0.0))
        if m == LAST:
            c_new = jnp.concatenate([stat[33, g:g + 1, :] for g in range(4)], axis=1)
            parts, row_total = stat[33, 4:5, 0:1], stat[33, 5:6, 0:1]
        else:
            c_new = jnp.concatenate([stat[TILE * (m % 5) + g, row:row + 1, :] for g in range(TILE)], axis=1)
            parts = sum(stat[TILE * (m % 5) + g, row + 2:row + 3, 0:1] for g in range(TILE))
        if m < 4:
            ac_new[m:m + 1, :] = c_new
        else:
            (ic_new, oc_new)[m - 4][...] = c_new
        w_sq = over_cols(jnp.where(lane == TILE + m, scal, 0.0))
        coeff = step_size(parts, w_sq, N_ROWS[m] * N_COLS[m])
        col_factor = lax.rsqrt(c_new)
        w = aw.at[m] if m < 4 else (iw, ow)[m - 4]
        for u in range(N_UNITS):
            if UNITS[u][0] != m:
                continue
            r_at, c_at = UNITS[u][1:]
            r_factor = lax.rsqrt(rows[ROW_AT[m] + r_at:ROW_AT[m] + r_at + BLK_R, 0:1] / (row_total / N_ROWS[m]))
            step = coeff * (gs_v[u] * r_factor * col_factor[:, c_at:c_at + BLK_C])
            part = (slice(r_at, r_at + BLK_R), slice(c_at, c_at + BLK_C))
            w[part] = w[part] - step
        if m >= 3:
            outs.append(pltpu.make_async_copy((aw, iw, ow)[m - 3], (aw_new, iw_new, ow_new)[m - 3],
                                              out_sem.at[m - 3]))
            outs[-1].start()
    for load, out in moves:
        load.wait()
        out.start()
        outs.append(out)
    for out in outs:
        out.wait()


def final_update(sums, dense_w):
    experts = [(1,) + shape if shape[0] > 1 else shape for shape in EXPERT_SHAPES]
    return pl.pallas_call(
        final_kernel,
        out_shape=shapes_of((4, N_DEV, D_MODEL), (4, N_DEV), (4, D_MODEL), (N_DEV, D_FF), (1, N_DEV), (1, D_FF), (16, D_MODEL), (1, 16),
                            (1, D_MODEL), *experts),
        in_specs=[ANY] * 12,
        out_specs=[ANY, VMEM, VMEM] * 3 + [ANY] * 6,
        scratch_shapes=[
            *[pltpu.VMEM(a.shape, F32) for a in (*sums[:3], *dense_w, *sums[3:])],
            pltpu.SemaphoreType.DMA((18,)), pltpu.SemaphoreType.DMA((15,)),
        ],
        compiler_params=pltpu.CompilerParams(vmem_limit_bytes=67043328),
        name="final_update",
    )(*sums[:3], *dense_w, *sums[3:])


def solution(mesh):
    dense_specs = (
        (P("dp"), P(None, "dp", None), P(None, "dp"), P()),
        (P("dp"), P("dp", None), P("dp"), P()),
        (P("dp"), P("dp", None), P("dp"), P()),
    )
    expert_specs = ((P("dp"), P("dp"), P("dp"), P("dp")),) * 2
    all_specs = dense_specs + expert_specs
    in_specs = tuple(part_spec for group in all_specs for part_spec in group)
    out_specs = tuple(part_spec for group in all_specs for part_spec in group[1:])

    def update_all(*arrays):
        (ag, aw, ar, ac, ig, iw, ir, ic, og, ow, orow, oc) = arrays[:12]
        grads = (ag.reshape(4, N_DEV, N_DEV, D_MODEL), ig.reshape(N_DEV, N_DEV, D_FF), og.reshape(N_DEV, 16, D_MODEL))
        sums = dense_sums(grads, (aw, iw, ow, ar, ir.reshape(1, N_DEV), orow.reshape(1, 16),
                                  ac, ic.reshape(1, D_FF), oc.reshape(1, D_MODEL)), arrays[12:])
        out = final_update(sums, (aw, iw, ow))
        return tuple(o.reshape(-1) if n in (4, 5, 7, TILE) else o for n, o in enumerate(out))

    return jax.shard_map(update_all, mesh=mesh, in_specs=in_specs, out_specs=out_specs, check_vma=False)
```

```python
import functools

import jax
import jax.numpy as jnp
from jax import lax
from jax.experimental import pallas as pl
from jax.experimental.pallas import tpu as pltpu
from jax.sharding import PartitionSpec as P

D_MODEL, D_FF, LANES, N_DEV, TILE = 1024, 512, 128, 32, 8
OPT_STEP = 10
LEARN_RATE = 0.1
EPS_SQUARE = 1e-30
EPS_SCALE = 1e-3
BETA_TWO = 1.0 - OPT_STEP ** -0.8
KEEP = 1.0 - BETA_TWO
F32 = jnp.float32
BLK_R, BLK_C = 16, D_FF
N_UNITS = 20
BIT = {"x": 1, "y": 2, "a": 3, "b": 4}

ORDERS = (
    "xayb", "yaxb", "ayxb", "ayxb", "xyab", "axyb", "xyab", "axyb", "xyab", "yxab",
    "yaxb", "yaxb", "xyab", "yxab", "axyb", "yxab", "axyb", "xayb", "yxab", "xyab",
)
STEP_UNITS = "".join((
    "DRFPQDRINGKPINQHRPMCHALGBKCOBQRFGHSAEJTQJBNOMFAICRNHDIBLEPMN",
    "CHRKFDPBGOIKEJQLGDCBOASFMKTIOJLADQMEJTHKLSEAMNCTGFLOJPSETSTS",
))
STEPS = [(ord(u) - ord("A"), STEP_UNITS[:n].count(u)) for n, u in enumerate(STEP_UNITS)]

UNITS = [(m, 16 * r, D_FF * c) for m in range(4) for r in range(2) for c in range(2)]
UNITS += [(5, 0, 0), (5, 0, D_FF), (4, 0, 0), (4, 16, 0)]
N_ROWS = (D_MODEL, D_MODEL, D_MODEL, D_MODEL, D_MODEL, D_FF)
N_COLS = (D_MODEL, D_MODEL, D_MODEL, D_MODEL, D_FF, D_MODEL)
LOC_ROWS = (N_DEV, N_DEV, N_DEV, N_DEV, N_DEV, 16)
ROW_AT = (0, N_DEV, 64, 96, LANES, 160)
LAST = 4
EARLY = 1
WORK_AT, WORK_EVERY = 16, 3
MESH = pl.DeviceIdType.MESH


def sum_of(value, axis):
    return jnp.sum(value, axis=axis, keepdims=True)


over_rows, over_cols = (functools.partial(sum_of, axis=axis) for axis in range(2))


def sum_all(value):
    return over_rows(over_cols(value))


def step_size(upd_sq, w_sq, n_elems):
    w_rms = jnp.sqrt(w_sq / n_elems)
    return LEARN_RATE * jnp.maximum(EPS_SCALE, w_rms) / jnp.maximum(1.0, jnp.sqrt(upd_sq / n_elems))


def expert_work(loads, arrays, results, sums, factor, acc):
    g_v, w_v, r_old, c_old = arrays
    r_new, c_new = results
    n_rows, n_cols = g_v.shape
    c_acc, w_acc, u_acc = (acc.at[n, :, pl.ds(0, n_cols)] for n in range(3))
    quarter = n_rows // 4

    def begin():
        for load in loads:
            load.wait()
        for ref in (c_acc, w_acc, u_acc):
            ref[...] = jnp.zeros((TILE, n_cols), F32)

    def squares(b):
        c_sum, w_sum = c_acc[...], w_acc[...]
        for r in range(16):
            at = slice(LANES * b + TILE * r, LANES * b + TILE * r + TILE)
            sq = g_v[at, :] * g_v[at, :] + EPS_SQUARE
            c_sum = c_sum + sq
            w_sum = w_sum + w_v[at, :] * w_v[at, :]
            sums[TILE * r:TILE * r + TILE, :] = jnp.broadcast_to(over_cols(sq), (TILE, LANES))
        c_acc[...], w_acc[...] = c_sum, w_sum
        part = slice(LANES * b, LANES * b + LANES)
        r_new[:, part] = BETA_TWO * r_old[:, part] + KEEP * (jnp.transpose(sums[...])[0:1, :] / n_cols)

    def factors():
        c_new[...] = BETA_TWO * c_old[...] + KEEP * (over_rows(c_acc[...]) / n_rows)
        mean = over_cols(r_new[...]) / n_rows
        row_factor = lax.rsqrt(r_new[...] / mean)
        for b in range(n_rows // LANES):
            part = slice(LANES * b, LANES * b + LANES)
            factor[part, :] = jnp.transpose(jnp.broadcast_to(row_factor[:, part], (LANES, LANES)))

    def update(q):
        col_factor = lax.rsqrt(c_new[...])

        @pl.loop(0, quarter // N_DEV)
        def _(n):
            at = pl.ds(q * quarter + n * N_DEV, N_DEV)
            upd = g_v[at, :] * factor[at, 0:1] * col_factor
            g_v[at, :] = upd
            sq = upd * upd
            u_acc[...] = u_acc[...] + sq[0:TILE] + sq[TILE:16] + sq[16:24] + sq[24:N_DEV]

    def finish(q):
        coeff = step_size(sum_all(u_acc[...]), sum_all(w_acc[...]), n_rows * n_cols)

        @pl.loop(0, quarter // N_DEV)
        def _(n):
            at = pl.ds(q * quarter + n * N_DEV, N_DEV)
            w_v[at, :] = w_v[at, :] - coeff * g_v[at, :]

    pieces = [begin] + [functools.partial(squares, b) for b in range(n_rows // LANES)] + [factors]
    return pieces + [functools.partial(f, q) for f in (update, finish) for q in range(4)]


def dense_kernel(attn_g, ffin_g, ffout_g, *refs):
    small, expert_in, refs = refs[:9], refs[9:17], refs[17:]
    (g_own, row_out, stat_out), dense_w, expert_out, scratch = refs[:3], refs[3:6], refs[6:12], refs[12:]
    small_vmem, (g_in, *states_in), (g_out, *states_out), scratch = (
        dense_w + scratch[:6], scratch[6:9], scratch[9:12], scratch[12:])
    expert_v = (g_in, expert_out[0], *states_in, g_out, expert_out[3], *states_out)
    raw, stage, r0, r1, r2, r3, r4, msg, rx, rb, rx_end, rx_row, tile, end, end_row, rows_msg, rx_rows, *scratch = scratch
    sums, factor, acc, ld_sem, s_sem, r_sem, x_sem, e_sem = scratch
    attn_w, ffin_w, ffout_w, attn_r, ffin_r, ffout_r, attn_c, ffin_c, ffout_c = small_vmem
    me = lax.axis_index("dp")
    bits = [(me // 2 ** k) % 2 for k in range(5)]
    partner = [me + (1 - 2 * bits[k]) * 2 ** k for k in range(5)]
    core = bits[0]
    recvs = (r0, r1, r2, r3, r4)

    def source(u):
        m, row, col = UNITS[u]
        if m < 4:
            return attn_g.at[m, :, pl.ds(row, BLK_R), pl.ds(col, BLK_C)]
        ref = ffin_g if m == 4 else ffout_g
        return ref.at[:, pl.ds(row, BLK_R), pl.ds(col, BLK_C)]

    barrier = pltpu.get_barrier_semaphore()
    for t in range(1, N_DEV):
        pl.semaphore_signal(barrier, inc=1, device_id=((me + t) % N_DEV,), device_id_type=MESH)
    loads = [pltpu.make_async_copy(source(u), raw.at[u], ld_sem.at[u]) for u in range(N_UNITS)]
    stage_zero = [u for u, s in STEPS if s == 0]
    for u in stage_zero[:2]:
        loads[u].start()
    small_loads = [pltpu.make_async_copy(a, b, ld_sem.at[N_UNITS]) for a, b in zip(small, small_vmem)]
    def dest(order, i):
        return sum(((i // 2 ** (3 - j)) % 2) * 2 ** BIT[order[j]] for j in range(4))

    def copy(u, s):
        order = ORDERS[u]
        if s == 0:
            src, to = stage.at[u], partner[0]
        else:
            keep = sum(bits[BIT[order[j]]] * 2 ** (3 - j) for j in range(s - 1))
            k = BIT[order[s - 1]]
            src = r0.at[u, pl.ds(keep + (1 - bits[k]) * 2 ** (4 - s), 2 ** (4 - s))]
            to = partner[k]
        return pltpu.make_async_remote_copy(
            src_ref=src, dst_ref=recvs[s].at[u], send_sem=s_sem.at[s], recv_sem=r_sem.at[s, u],
            device_id=(to,), device_id_type=MESH)

    def block_sum(u, s, i, d):
        total = raw[u, d].astype(F32)
        for j in range(s):
            total = total + recvs[j][u, i % 2 ** (4 - j)]
        return total

    rows_in = (attn_r, attn_r, attn_r, attn_r, ffin_r, ffout_r)
    weights = (attn_w, attn_w, attn_w, attn_w, ffin_w, ffout_w)
    lane = lax.broadcasted_iota(jnp.int32, (1, LANES), 1)

    def statistics(m):
        n_loc, n_col = LOC_ROWS[m], N_COLS[m]
        col_s, col_d = ([0.0] * (n_col // D_FF) for _ in range(2))
        new_rows = []
        total = jnp.zeros((1, 1), F32)
        for h in range(n_loc // 16):
            here = [u for u in range(N_UNITS) if UNITS[u][:2] == (m, 16 * h)]
            squares = {u: g_own[u] * g_own[u] for u in here}
            row_sum = sum(over_cols(squares[u] + EPS_SQUARE) for u in here)
            old = rows_in[m][m:m + 1, :] if m < 4 else rows_in[m][...]
            pick = lax.broadcasted_iota(jnp.int32, (16, n_loc), 0) + 16 * h == lax.broadcasted_iota(
                jnp.int32, (16, n_loc), 1)
            old_col = over_cols(jnp.where(pick, jnp.broadcast_to(old, (16, n_loc)), 0.0))
            new = BETA_TWO * old_col + KEEP * (row_sum / n_col)
            row_out[pl.ds(ROW_AT[m] + 16 * h, 16), :] = jnp.broadcast_to(new, (16, LANES))
            total = total + over_rows(new)
            new_rows.append((new, here, squares))
        mean = total / n_loc
        for new, here, squares in new_rows:
            inv = mean / new
            for u in here:
                c = UNITS[u][2] // D_FF
                col_s[c] = col_s[c] + over_rows(squares[u] + EPS_SQUARE)
                col_d[c] = col_d[c] + over_rows(squares[u] * inv)
        return total, col_s, col_d

    z, rest = me // TILE, me % TILE
    z_order = [TILE * (3 - z), TILE * ((z + 2) % 4), TILE * (z + 1 - 2 * (z % 2)), TILE * z]

    def exchange(k, src_of, dst):
        for n, at in enumerate(z_order):
            @pl.loop(n // 3, TILE)
            def _(r, at=at):
                to = at + (rest + r) % TILE
                pltpu.make_async_remote_copy(
                    src_ref=src_of(to), dst_ref=dst.at[me], send_sem=x_sem.at[2 * k], recv_sem=x_sem.at[2 * k + 1],
                    device_id=(to,), device_id_type=MESH).start()

    def wait_all(sem, dst):
        some = dst.at[pl.ds(0, 31)]
        pltpu.make_async_copy(some, some, x_sem.at[sem]).wait()

    def collect_weights():
        rows_msg[...] = sum(jnp.where(lane == TILE + m, sum_all(w * w), 0.0)
                            for m, w in enumerate(weights[m][m] if m < 4 else weights[m][...] for m in range(6)))
        msg[...] = jnp.zeros((N_DEV, 4, LANES), F32)

    def collect(m):
        total, col_s, col_d = statistics(m)
        for g in range(TILE):
            at = TILE * (m % 5) + g
            row = 0 if m < 4 else 2
            part = slice(LANES * (g % 4), LANES * (g % 4) + LANES)
            msg[at, row:row + 1, :] = col_s[g // 4][:, part]
            msg[at, row + 1:row + 2, :] = col_d[g // 4][:, part]
        rows_msg[...] = rows_msg[...] + jnp.where(lane == m, total, 0.0)

    def send_first():
        exchange(0, lambda to: msg.at[to], rx)
        exchange(4, lambda to: rows_msg, rx_rows)
        rx[me] = msg[me]
        rx_rows[me] = rows_msg[...]

    def lanes_at(k):
        return pl.ds(pl.multiple_of(k * LANES, LANES), LANES)

    def own_groups():
        wait_all(1, rx)
        wait_all(9, rx_rows)
        scal = rx_rows[:, 0, :]
        lanes = lax.broadcasted_iota(jnp.int32, (N_DEV, LANES), 1)

        def group(row, mat, n_row, old):
            sums = over_cols(jnp.where(lanes == mat, scal, 0.0))
            ratio = over_rows(sums) / 32.0 / sums
            new = BETA_TWO * old + KEEP * (over_rows(rx[:, row, :]) / n_row)
            part = over_cols(over_rows(rx[:, row + 1, :] * ratio) / new)
            tile[row // 2:row // 2 + 1, :] = new
            tile[row // 2 + 2:row // 2 + 3, :] = jnp.broadcast_to(part, (1, LANES))

        here = lanes_at(me % TILE)
        group(0, me // TILE, 1024.0, sum(jnp.where(me // TILE == m, attn_c[m:m + 1, here], 0.0) for m in range(4)))
        group(2, 5, 512.0, ffout_c[:, here])
        exchange(1, lambda to: tile, rb)
        rb[me] = tile[...]
        stat_out[N_DEV, 0:1, :] = over_rows(scal)

    def send_last():
        total, (col_s,), (col_d,) = statistics(LAST)
        for g in range(4):
            part = slice(LANES * g, LANES * g + LANES)
            end[g:g + 1, :] = col_s[:, part]
            end[g + 4:g + 5, :] = col_d[:, part]
        end_row[...] = jnp.broadcast_to(total, (1, LANES))
        exchange(2, lambda to: end, rx_end)
        exchange(3, lambda to: end_row, rx_row)
        rx_end[me] = end[...]
        rx_row[me] = end_row[...]

    def take_last():
        wait_all(5, rx_end)
        wait_all(7, rx_row)
        rows_all = rx_row[:, 0, :]
        grand = over_rows(rows_all)
        ratio = grand / 32.0 / rows_all
        is_s = lax.broadcasted_iota(jnp.int32, (TILE, LANES), 0) < 4
        both = [jnp.zeros((TILE, LANES), F32) for _ in range(4)]
        for p in range(N_DEV):
            both[p % 4] = both[p % 4] + rx_end[p] * jnp.where(is_s, 1.0, ratio[p:p + 1, :])
        both = (both[0] + both[1]) + (both[2] + both[3])
        col_s, col_d = both[0:4, :], both[4:TILE, :]
        for g in range(4):
            stat_out[33, g:g + 1, :] = ffin_c[:, LANES * g:LANES * g + LANES]
        new = BETA_TWO * stat_out[33, 0:4, :] + KEEP * (col_s / 1024.0)
        stat_out[33, 0:4, :] = new
        stat_out[33, 4:5, :] = jnp.broadcast_to(sum_all(col_d / new), (1, LANES))
        stat_out[33, 5:6, :] = grand

    def to_f32(u):
        loads[u].wait()

        @pl.loop(0, 4)
        def _(n):
            for k in range(4):
                i = 4 * n + k
                stage[u, i] = raw[u, dest(ORDERS[u], i) + 1 - core].astype(F32)

    def step(u, s):
        order = ORDERS[u]
        if s == 0:
            to_f32(u)
        else:
            copy(u, s - 1).wait_recv()
            base = sum(bits[BIT[order[j]]] * 2 ** (3 - j) for j in range(min(s - 1, 4)))
            if s == 5:
                g_own[u] = block_sum(u, 5, base, me) * (1.0 / 32.0)
                return
            base = base + (1 - bits[BIT[order[s - 1]]]) * 2 ** (4 - s)

            @pl.loop(0, 2 ** (4 - s))
            def _(n):
                i = base + n
                r0[u, i] = block_sum(u, s, i, dest(order, i) + core)
        copy(u, s).start()

    for u in stage_zero[2:TILE]:
        loads[u].start()
    for u in stage_zero[:EARLY]:
        to_f32(u)
    pl.semaphore_wait(barrier, 31)
    for u in stage_zero[:EARLY]:
        copy(u, 0).start()
    for u in stage_zero[TILE:]:
        loads[u].start()
    expert_loads = [pltpu.make_async_copy(a.at[0] if n % 4 < 2 else a, b, e_sem.at[n])
                    for n, (a, b) in enumerate(zip(expert_in, expert_v))]
    work = []
    for k in range(2):
        half = slice(4 * k, 4 * k + 4)
        work += expert_work(expert_loads[half], expert_v[half], expert_out[3 * k + 1:3 * k + 3], sums, factor, acc.at[k])
    left = {m: sum(unit[0] == m for unit in UNITS) for m in range(6)}
    for n, (u, s) in enumerate(STEPS):
        if n == WORK_AT - 4:
            for load in small_loads + expert_loads:
                load.start()
            for load in small_loads:
                load.wait()
            collect_weights()
        if s > 0 or u not in stage_zero[:EARLY]:
            step(u, s)
        if n >= WORK_AT and n % WORK_EVERY == 0 and work:
            work.pop(0)()
        if n == len(STEPS) - TILE:
            for piece in work:
                piece()
        if s == 5:
            m = UNITS[u][0]
            left[m] -= 1
            if left[m] == 0 and m != LAST:
                collect(m)
            if s == 5 and sum(left.values()) == left[LAST] and m != LAST:
                send_first()
    send_last()
    own_groups()

    for k, sent in enumerate((stage, r1, r2, r3, r4)):
        pltpu.make_async_copy(sent, sent, s_sem.at[k]).wait()
    take_last()
    wait_all(3, rb)
    stat_out[pl.ds(0, N_DEV), 0:4, :] = rb[...]
    for k, ref in ((0, msg), (2, rb), (4, rx_end), (6, rx_row), (TILE, rx_rows)):
        wait_all(k, ref)


ANY = pl.BlockSpec(memory_space=pl.ANY)
VMEM = pl.BlockSpec(memory_space=pltpu.VMEM)


EXPERT_SHAPES = ((D_MODEL, D_FF), (1, D_MODEL), (1, D_FF), (D_FF, D_MODEL), (1, D_FF), (1, D_MODEL))


def shapes_of(*shapes):
    return tuple(jax.ShapeDtypeStruct(shape, F32) for shape in shapes)


def in_vmem(*shapes):
    return tuple(pltpu.VMEM(shape, F32) for shape in shapes)


def dense_sums(grads, small, experts):
    block = (BLK_R, BLK_C)
    halves = [pltpu.VMEM((N_UNITS, 2 ** k) + block, F32) for k in (4, 4, 3, 2, 1, 0)]
    return pl.pallas_call(
        dense_kernel,
        out_shape=in_vmem((N_UNITS,) + block, (176, LANES), (34, TILE, LANES), *[a.shape for a in small[:3]], *EXPERT_SHAPES),
        in_specs=[ANY] * 20,
        out_specs=(VMEM,) * 12,
        scratch_shapes=[pltpu.VMEM(a.shape, F32) for a in small[3:]] + [
            pltpu.VMEM(a.shape[-2:], F32) for n, a in enumerate(experts) if n % 4 != 1] + [
            pltpu.VMEM((N_UNITS, N_DEV) + block, jnp.bfloat16), *halves,
            *[pltpu.VMEM((N_DEV, 4, LANES), F32)] * 3, pltpu.VMEM((N_DEV, TILE, LANES), F32), pltpu.VMEM((N_DEV, 1, LANES), F32),
            pltpu.VMEM((4, LANES), F32), pltpu.VMEM((TILE, LANES), F32), pltpu.VMEM((1, LANES), F32),
            pltpu.VMEM((1, LANES), F32), pltpu.VMEM((N_DEV, 1, LANES), F32),
            pltpu.VMEM((LANES, LANES), F32), pltpu.VMEM((D_MODEL, LANES), F32), pltpu.VMEM((2, 3, TILE, D_MODEL), F32),
            pltpu.SemaphoreType.DMA((N_UNITS + 1,)),
            pltpu.SemaphoreType.DMA((5,)), pltpu.SemaphoreType.DMA((5, N_UNITS)),
            pltpu.SemaphoreType.DMA((10,)),
            pltpu.SemaphoreType.DMA((TILE,)),
        ],
        compiler_params=pltpu.CompilerParams(
            has_side_effects=True, vmem_limit_bytes=52 * 2 ** 20, collective_id=1),
        name="dense_sums",
    )(*grads, *small, *experts)


def final_kernel(gs_v, rows, stat, *refs):
    (aw, iw, ow), expert_in, refs = refs[:3], refs[3:9], refs[9:]
    (aw_new, ar_new, ac_new, iw_new, ir_new, ic_new, ow_new, or_new, oc_new), refs = refs[:9], refs[9:]
    expert_out, updated, out_sem = refs[:6], refs[6:9], refs[9]

    outs = [pltpu.make_async_copy(a, b if k % 3 else b.at[0], out_sem.at[3 + k])
            for k, (a, b) in enumerate(zip(expert_in, expert_out))]
    for out in outs:
        out.start()

    scal = stat[N_DEV, 0:1, :]
    lane = lax.broadcasted_iota(jnp.int32, (1, LANES), 1)
    flipped = (jnp.transpose(rows[0:LANES, :]), jnp.transpose(rows[48:176, :]))
    for m in range(4):
        ar_new[m:m + 1, :] = flipped[0][0:1, N_DEV * m:N_DEV * m + N_DEV]
    ir_new[...] = flipped[1][0:1, 80:112]
    or_new[...] = flipped[1][0:1, 112:LANES]
    for m in range(6):
        row = m // 5
        row_total = over_cols(jnp.where(lane == m, scal, 0.0))
        if m == LAST:
            c_new = jnp.concatenate([stat[33, g:g + 1, :] for g in range(4)], axis=1)
            parts, row_total = stat[33, 4:5, 0:1], stat[33, 5:6, 0:1]
        else:
            c_new = jnp.concatenate([stat[TILE * (m % 5) + g, row:row + 1, :] for g in range(TILE)], axis=1)
            parts = sum(stat[TILE * (m % 5) + g, row + 2:row + 3, 0:1] for g in range(TILE))
        if m < 4:
            ac_new[m:m + 1, :] = c_new
        else:
            (ic_new, oc_new)[m - 4][...] = c_new
        w_sq = over_cols(jnp.where(lane == TILE + m, scal, 0.0))
        coeff = step_size(parts, w_sq, N_ROWS[m] * N_COLS[m])
        col_factor = lax.rsqrt(c_new)
        w = aw.at[m] if m < 4 else (iw, ow)[m - 4]
        for u in range(N_UNITS):
            if UNITS[u][0] != m:
                continue
            r_at, c_at = UNITS[u][1:]
            r_factor = lax.rsqrt(rows[ROW_AT[m] + r_at:ROW_AT[m] + r_at + BLK_R, 0:1] / (row_total / N_ROWS[m]))
            step = coeff * (gs_v[u] * r_factor * col_factor[:, c_at:c_at + BLK_C])
            part = (slice(r_at, r_at + BLK_R), slice(c_at, c_at + BLK_C))
            new = updated[0].at[m] if m < 4 else updated[m - 3]
            new[part] = w[part] - step
        if m >= 3:
            outs.append(pltpu.make_async_copy(updated[m - 3], (aw_new, iw_new, ow_new)[m - 3], out_sem.at[m - 3]))
            outs[-1].start()
    for out in outs:
        out.wait()


def final_update(sums):
    experts = [(1,) + shape if shape[0] > 1 else shape for shape in EXPERT_SHAPES]
    return pl.pallas_call(
        final_kernel,
        out_shape=shapes_of((4, N_DEV, D_MODEL), (4, N_DEV), (4, D_MODEL), (N_DEV, D_FF), (1, N_DEV), (1, D_FF), (16, D_MODEL), (1, 16),
                            (1, D_MODEL), *experts),
        in_specs=[VMEM] * 12,
        out_specs=[ANY, VMEM, VMEM] * 3 + [ANY] * 6,
        scratch_shapes=[*in_vmem(*[a.shape for a in sums[3:6]]), pltpu.SemaphoreType.DMA((9,))],
        compiler_params=pltpu.CompilerParams(vmem_limit_bytes=TILE * 2 ** 20),
        name="final_update",
    )(*sums)


def solution(mesh):
    dense_specs = (
        (P("dp"), P(None, "dp", None), P(None, "dp"), P()),
        (P("dp"), P("dp", None), P("dp"), P()),
        (P("dp"), P("dp", None), P("dp"), P()),
    )
    expert_specs = ((P("dp"), P("dp"), P("dp"), P("dp")),) * 2
    all_specs = dense_specs + expert_specs
    in_specs = tuple(part_spec for group in all_specs for part_spec in group)
    out_specs = tuple(part_spec for group in all_specs for part_spec in group[1:])

    def update_all(*arrays):
        (ag, aw, ar, ac, ig, iw, ir, ic, og, ow, orow, oc) = arrays[:12]
        grads = (ag.reshape(4, N_DEV, N_DEV, D_MODEL), ig.reshape(N_DEV, N_DEV, D_FF), og.reshape(N_DEV, 16, D_MODEL))
        sums = dense_sums(grads, (aw, iw, ow, ar, ir.reshape(1, N_DEV), orow.reshape(1, 16),
                                  ac, ic.reshape(1, D_FF), oc.reshape(1, D_MODEL)), arrays[12:])
        out = final_update(sums)
        return tuple(o.reshape(-1) if n in (4, 5, 7, TILE) else o for n, o in enumerate(out))

    return jax.shard_map(update_all, mesh=mesh, in_specs=in_specs, out_specs=out_specs, check_vma=False)
```

```python
import functools

import jax
import jax.numpy as jnp
from jax import lax
from jax.experimental import pallas as pl
from jax.experimental.pallas import tpu as pltpu
from jax.sharding import PartitionSpec as P

D_MODEL, D_FF, LANES, N_DEV, TILE = 1024, 512, 128, 32, 8
OPT_STEP = 10
LEARN_RATE = 0.1
EPS_SQUARE = 1e-30
EPS_SCALE = 1e-3
BETA_TWO = 1.0 - OPT_STEP ** -0.8
KEEP = 1.0 - BETA_TWO
F32 = jnp.float32
BLK_R, BLK_C = 16, D_FF
N_UNITS = 20
BIT = {"x": 1, "y": 2, "a": 3, "b": 4}

ORDERS = (
    "xyab", "yaxb", "xyab", "xayb", "xyab", "yxab", "ayxb", "axyb", "yaxb", "yaxb",
    "ayxb", "yaxb", "xyab", "xayb", "ayxb", "xayb", "ayxb", "xyab", "xyab", "yxab",
)
STEP_UNITS = "".join((
    "NHFIMJNBHFQMQJLNKROHAROBACJFITKLGNGECDDHJKPELAFNMGIBDHCLKIAQ",
    "PBFGMEORLCAJTQSEMLCSKIPEDBRAOQMPGNTDCRSOFIPJGTDHBQKRSEOPTSTS",
))
STEPS = [(ord(u) - ord("A"), STEP_UNITS[:n].count(u)) for n, u in enumerate(STEP_UNITS)]

UNITS = [(m, 16 * r, D_FF * c) for m in range(4) for r in range(2) for c in range(2)]
UNITS += [(5, 0, 0), (5, 0, D_FF), (4, 0, 0), (4, 16, 0)]
N_ROWS = (D_MODEL, D_MODEL, D_MODEL, D_MODEL, D_MODEL, D_FF)
N_COLS = (D_MODEL, D_MODEL, D_MODEL, D_MODEL, D_FF, D_MODEL)
LOC_ROWS = (N_DEV, N_DEV, N_DEV, N_DEV, N_DEV, 16)
ROW_AT = (0, N_DEV, 64, 96, LANES, 160)
LAST = 4
EARLY = 2
WORK_AT, WORK_EVERY = 16, 3
MESH = pl.DeviceIdType.MESH


def sum_of(value, axis):
    return jnp.sum(value, axis=axis, keepdims=True)


over_rows, over_cols = (functools.partial(sum_of, axis=axis) for axis in range(2))


def sum_all(value):
    return over_rows(over_cols(value))


def step_size(upd_sq, w_sq, n_elems):
    w_rms = jnp.sqrt(w_sq / n_elems)
    return LEARN_RATE * jnp.maximum(EPS_SCALE, w_rms) / jnp.maximum(1.0, jnp.sqrt(upd_sq / n_elems))


def expert_work(loads, arrays, results, sums, factor, acc):
    g_v, w_v, r_old, c_old = arrays
    r_new, c_new = results
    n_rows, n_cols = g_v.shape
    c_acc, w_acc, u_acc = (acc.at[n, :, pl.ds(0, n_cols)] for n in range(3))
    quarter = n_rows // 4

    def begin():
        for load in loads:
            load.wait()
        for ref in (c_acc, w_acc, u_acc):
            ref[...] = jnp.zeros((TILE, n_cols), F32)

    def squares(b):
        c_sum, w_sum = c_acc[...], w_acc[...]
        for r in range(16):
            at = slice(LANES * b + TILE * r, LANES * b + TILE * r + TILE)
            sq = g_v[at, :] * g_v[at, :] + EPS_SQUARE
            c_sum = c_sum + sq
            w_sum = w_sum + w_v[at, :] * w_v[at, :]
            sums[TILE * r:TILE * r + TILE, :] = jnp.broadcast_to(over_cols(sq), (TILE, LANES))
        c_acc[...], w_acc[...] = c_sum, w_sum
        part = slice(LANES * b, LANES * b + LANES)
        r_new[:, part] = BETA_TWO * r_old[:, part] + KEEP * (jnp.transpose(sums[...])[0:1, :] / n_cols)

    def factors():
        c_new[...] = BETA_TWO * c_old[...] + KEEP * (over_rows(c_acc[...]) / n_rows)
        mean = over_cols(r_new[...]) / n_rows
        row_factor = lax.rsqrt(r_new[...] / mean)
        for b in range(n_rows // LANES):
            part = slice(LANES * b, LANES * b + LANES)
            factor[part, :] = jnp.transpose(jnp.broadcast_to(row_factor[:, part], (LANES, LANES)))

    def update(q):
        col_factor = lax.rsqrt(c_new[...])

        @pl.loop(0, quarter // N_DEV)
        def _(n):
            at = pl.ds(q * quarter + n * N_DEV, N_DEV)
            upd = g_v[at, :] * factor[at, 0:1] * col_factor
            g_v[at, :] = upd
            sq = upd * upd
            u_acc[...] = u_acc[...] + sq[0:TILE] + sq[TILE:16] + sq[16:24] + sq[24:N_DEV]

    def finish(q):
        coeff = step_size(sum_all(u_acc[...]), sum_all(w_acc[...]), n_rows * n_cols)

        @pl.loop(0, quarter // N_DEV)
        def _(n):
            at = pl.ds(q * quarter + n * N_DEV, N_DEV)
            w_v[at, :] = w_v[at, :] - coeff * g_v[at, :]

    pieces = [begin] + [functools.partial(squares, b) for b in range(n_rows // LANES)] + [factors]
    return pieces + [functools.partial(f, q) for f in (update, finish) for q in range(4)]


def dense_kernel(attn_g, ffin_g, ffout_g, *refs):
    small, expert_in, refs = refs[:9], refs[9:17], refs[17:]
    (g_own, row_out, stat_out), dense_w, expert_out, scratch = refs[:3], refs[3:6], refs[6:12], refs[12:]
    small_vmem, (g_in, *states_in), (g_out, *states_out), scratch = (
        dense_w + scratch[:6], scratch[6:9], scratch[9:12], scratch[12:])
    expert_v = (g_in, expert_out[0], *states_in, g_out, expert_out[3], *states_out)
    raw, stage, r0, r1, r2, r3, r4, msg, rx, rb, rx_end, rx_row, tile, end, end_row, rows_msg, rx_rows, *scratch = scratch
    sums, factor, acc, ld_sem, s_sem, r_sem, x_sem, e_sem = scratch
    attn_w, ffin_w, ffout_w, attn_r, ffin_r, ffout_r, attn_c, ffin_c, ffout_c = small_vmem
    me = lax.axis_index("dp")
    bits = [(me // 2 ** k) % 2 for k in range(5)]
    partner = [me + (1 - 2 * bits[k]) * 2 ** k for k in range(5)]
    core = bits[0]
    recvs = (r0, r1, r2, r3, r4)

    def source(u):
        m, row, col = UNITS[u]
        if m < 4:
            return attn_g.at[m, :, pl.ds(row, BLK_R), pl.ds(col, BLK_C)]
        ref = ffin_g if m == 4 else ffout_g
        return ref.at[:, pl.ds(row, BLK_R), pl.ds(col, BLK_C)]

    barrier = pltpu.get_barrier_semaphore()
    for t in range(1, N_DEV):
        pl.semaphore_signal(barrier, inc=1, device_id=((me + t) % N_DEV,), device_id_type=MESH)
    loads = [pltpu.make_async_copy(source(u), raw.at[u], ld_sem.at[u]) for u in range(N_UNITS)]
    stage_zero = [u for u, s in STEPS if s == 0]
    for u in stage_zero[:2]:
        loads[u].start()
    small_loads = [pltpu.make_async_copy(a, b, ld_sem.at[N_UNITS]) for a, b in zip(small, small_vmem)]
    def dest(order, i):
        return sum(((i // 2 ** (3 - j)) % 2) * 2 ** BIT[order[j]] for j in range(4))

    def copy(u, s):
        order = ORDERS[u]
        if s == 0:
            src, to = stage.at[u], partner[0]
        else:
            keep = sum(bits[BIT[order[j]]] * 2 ** (3 - j) for j in range(s - 1))
            k = BIT[order[s - 1]]
            src = r0.at[u, pl.ds(keep + (1 - bits[k]) * 2 ** (4 - s), 2 ** (4 - s))]
            to = partner[k]
        return pltpu.make_async_remote_copy(
            src_ref=src, dst_ref=recvs[s].at[u], send_sem=s_sem.at[s], recv_sem=r_sem.at[s, u],
            device_id=(to,), device_id_type=MESH)

    def block_sum(u, s, i, d):
        total = raw[u, d].astype(F32)
        for j in range(s):
            total = total + recvs[j][u, i % 2 ** (4 - j)]
        return total

    rows_in = (attn_r, attn_r, attn_r, attn_r, ffin_r, ffout_r)
    weights = (attn_w, attn_w, attn_w, attn_w, ffin_w, ffout_w)
    lane = lax.broadcasted_iota(jnp.int32, (1, LANES), 1)

    def statistics(m):
        n_loc, n_col = LOC_ROWS[m], N_COLS[m]
        col_s, col_d = ([0.0] * (n_col // D_FF) for _ in range(2))
        new_rows = []
        total = jnp.zeros((1, 1), F32)
        for h in range(n_loc // 16):
            here = [u for u in range(N_UNITS) if UNITS[u][:2] == (m, 16 * h)]
            squares = {u: g_own[u] * g_own[u] for u in here}
            row_sum = sum(over_cols(squares[u] + EPS_SQUARE) for u in here)
            old = rows_in[m][m:m + 1, :] if m < 4 else rows_in[m][...]
            pick = lax.broadcasted_iota(jnp.int32, (16, n_loc), 0) + 16 * h == lax.broadcasted_iota(
                jnp.int32, (16, n_loc), 1)
            old_col = over_cols(jnp.where(pick, jnp.broadcast_to(old, (16, n_loc)), 0.0))
            new = BETA_TWO * old_col + KEEP * (row_sum / n_col)
            row_out[pl.ds(ROW_AT[m] + 16 * h, 16), :] = jnp.broadcast_to(new, (16, LANES))
            total = total + over_rows(new)
            new_rows.append((new, here, squares))
        mean = total / n_loc
        for new, here, squares in new_rows:
            inv = mean / new
            for u in here:
                c = UNITS[u][2] // D_FF
                col_s[c] = col_s[c] + over_rows(squares[u] + EPS_SQUARE)
                col_d[c] = col_d[c] + over_rows(squares[u] * inv)
        return total, col_s, col_d

    z, rest = me // TILE, me % TILE
    z_order = [TILE * (3 - z), TILE * ((z + 2) % 4), TILE * (z + 1 - 2 * (z % 2)), TILE * z]

    def exchange(k, src_of, dst):
        for n, at in enumerate(z_order):
            @pl.loop(n // 3, TILE)
            def _(r, at=at):
                to = at + (rest + r) % TILE
                pltpu.make_async_remote_copy(
                    src_ref=src_of(to), dst_ref=dst.at[me], send_sem=x_sem.at[2 * k], recv_sem=x_sem.at[2 * k + 1],
                    device_id=(to,), device_id_type=MESH).start()

    def wait_all(sem, dst):
        some = dst.at[pl.ds(0, 31)]
        pltpu.make_async_copy(some, some, x_sem.at[sem]).wait()

    def collect_weights():
        rows_msg[...] = sum(jnp.where(lane == TILE + m, sum_all(w * w), 0.0)
                            for m, w in enumerate(weights[m][m] if m < 4 else weights[m][...] for m in range(6)))
        msg[...] = jnp.zeros((N_DEV, 4, LANES), F32)

    def collect(m):
        total, col_s, col_d = statistics(m)
        for g in range(TILE):
            at = TILE * (m % 5) + g
            row = 0 if m < 4 else 2
            part = slice(LANES * (g % 4), LANES * (g % 4) + LANES)
            msg[at, row:row + 1, :] = col_s[g // 4][:, part]
            msg[at, row + 1:row + 2, :] = col_d[g // 4][:, part]
        rows_msg[...] = rows_msg[...] + jnp.where(lane == m, total, 0.0)

    def send_first():
        exchange(0, lambda to: msg.at[to], rx)
        exchange(4, lambda to: rows_msg, rx_rows)
        rx[me] = msg[me]
        rx_rows[me] = rows_msg[...]

    def lanes_at(k):
        return pl.ds(pl.multiple_of(k * LANES, LANES), LANES)

    def own_groups():
        wait_all(1, rx)
        wait_all(9, rx_rows)
        scal = rx_rows[:, 0, :]
        lanes = lax.broadcasted_iota(jnp.int32, (N_DEV, LANES), 1)

        def group(row, mat, n_row, old):
            sums = over_cols(jnp.where(lanes == mat, scal, 0.0))
            ratio = over_rows(sums) / 32.0 / sums
            new = BETA_TWO * old + KEEP * (over_rows(rx[:, row, :]) / n_row)
            part = over_cols(over_rows(rx[:, row + 1, :] * ratio) / new)
            tile[row // 2:row // 2 + 1, :] = new
            tile[row // 2 + 2:row // 2 + 3, :] = jnp.broadcast_to(part, (1, LANES))

        here = lanes_at(me % TILE)
        group(0, me // TILE, 1024.0, sum(jnp.where(me // TILE == m, attn_c[m:m + 1, here], 0.0) for m in range(4)))
        group(2, 5, 512.0, ffout_c[:, here])
        exchange(1, lambda to: tile, rb)
        rb[me] = tile[...]
        stat_out[N_DEV, 0:1, :] = over_rows(scal)

    def send_last():
        total, (col_s,), (col_d,) = statistics(LAST)
        for g in range(4):
            part = slice(LANES * g, LANES * g + LANES)
            end[g:g + 1, :] = col_s[:, part]
            end[g + 4:g + 5, :] = col_d[:, part]
        end_row[...] = jnp.broadcast_to(total, (1, LANES))
        exchange(2, lambda to: end, rx_end)
        exchange(3, lambda to: end_row, rx_row)
        rx_end[me] = end[...]
        rx_row[me] = end_row[...]

    def take_last():
        wait_all(5, rx_end)
        wait_all(7, rx_row)
        rows_all = rx_row[:, 0, :]
        grand = over_rows(rows_all)
        ratio = grand / 32.0 / rows_all
        is_s = lax.broadcasted_iota(jnp.int32, (TILE, LANES), 0) < 4
        both = [jnp.zeros((TILE, LANES), F32) for _ in range(4)]
        for p in range(N_DEV):
            both[p % 4] = both[p % 4] + rx_end[p] * jnp.where(is_s, 1.0, ratio[p:p + 1, :])
        both = (both[0] + both[1]) + (both[2] + both[3])
        col_s, col_d = both[0:4, :], both[4:TILE, :]
        for g in range(4):
            stat_out[33, g:g + 1, :] = ffin_c[:, LANES * g:LANES * g + LANES]
        new = BETA_TWO * stat_out[33, 0:4, :] + KEEP * (col_s / 1024.0)
        stat_out[33, 0:4, :] = new
        stat_out[33, 4:5, :] = jnp.broadcast_to(sum_all(col_d / new), (1, LANES))
        stat_out[33, 5:6, :] = grand

    def to_f32(u):
        loads[u].wait()

        @pl.loop(0, 4)
        def _(n):
            for k in range(4):
                i = 4 * n + k
                stage[u, i] = raw[u, dest(ORDERS[u], i) + 1 - core].astype(F32)

    def step(u, s):
        order = ORDERS[u]
        if s == 0:
            to_f32(u)
        else:
            copy(u, s - 1).wait_recv()
            base = sum(bits[BIT[order[j]]] * 2 ** (3 - j) for j in range(min(s - 1, 4)))
            if s == 5:
                g_own[u] = block_sum(u, 5, base, me) * (1.0 / 32.0)
                return
            base = base + (1 - bits[BIT[order[s - 1]]]) * 2 ** (4 - s)

            @pl.loop(0, 2 ** (4 - s))
            def _(n):
                i = base + n
                r0[u, i] = block_sum(u, s, i, dest(order, i) + core)
        copy(u, s).start()

    for u in stage_zero[2:TILE]:
        loads[u].start()
    for u in stage_zero[:EARLY]:
        to_f32(u)
    pl.semaphore_wait(barrier, 31)
    for u in stage_zero[:EARLY]:
        copy(u, 0).start()
    for u in stage_zero[TILE:]:
        loads[u].start()
    expert_loads = [pltpu.make_async_copy(a.at[0] if n % 4 < 2 else a, b, e_sem.at[n])
                    for n, (a, b) in enumerate(zip(expert_in, expert_v))]
    work = []
    for k in range(2):
        half = slice(4 * k, 4 * k + 4)
        work += expert_work(expert_loads[half], expert_v[half], expert_out[3 * k + 1:3 * k + 3], sums, factor, acc.at[k])
    left = {m: sum(unit[0] == m for unit in UNITS) for m in range(6)}
    for n, (u, s) in enumerate(STEPS):
        if n == WORK_AT - 4:
            for load in small_loads + expert_loads:
                load.start()
            for load in small_loads:
                load.wait()
            collect_weights()
        if s > 0 or u not in stage_zero[:EARLY]:
            step(u, s)
        if n >= WORK_AT and n % WORK_EVERY == 0 and work:
            work.pop(0)()
        if n == len(STEPS) - TILE:
            for piece in work:
                piece()
        if s == 5:
            m = UNITS[u][0]
            left[m] -= 1
            if left[m] == 0 and m != LAST:
                collect(m)
            if s == 5 and sum(left.values()) == left[LAST] and m != LAST:
                send_first()
    send_last()
    own_groups()

    for k, sent in enumerate((stage, r1, r2, r3, r4)):
        pltpu.make_async_copy(sent, sent, s_sem.at[k]).wait()
    take_last()
    wait_all(3, rb)
    stat_out[pl.ds(0, N_DEV), 0:4, :] = rb[...]
    for k, ref in ((0, msg), (2, rb), (4, rx_end), (6, rx_row), (TILE, rx_rows)):
        wait_all(k, ref)


ANY = pl.BlockSpec(memory_space=pl.ANY)
VMEM = pl.BlockSpec(memory_space=pltpu.VMEM)


EXPERT_SHAPES = ((D_MODEL, D_FF), (1, D_MODEL), (1, D_FF), (D_FF, D_MODEL), (1, D_FF), (1, D_MODEL))


def shapes_of(*shapes):
    return tuple(jax.ShapeDtypeStruct(shape, F32) for shape in shapes)


def in_vmem(*shapes):
    return tuple(pltpu.VMEM(shape, F32) for shape in shapes)


def dense_sums(grads, small, experts):
    block = (BLK_R, BLK_C)
    halves = [pltpu.VMEM((N_UNITS, 2 ** k) + block, F32) for k in (4, 4, 3, 2, 1, 0)]
    return pl.pallas_call(
        dense_kernel,
        out_shape=in_vmem((N_UNITS,) + block, (176, LANES), (34, TILE, LANES), *[a.shape for a in small[:3]], *EXPERT_SHAPES),
        in_specs=[ANY] * 20,
        out_specs=(VMEM,) * 12,
        scratch_shapes=[pltpu.VMEM(a.shape, F32) for a in small[3:]] + [
            pltpu.VMEM(a.shape[-2:], F32) for n, a in enumerate(experts) if n % 4 != 1] + [
            pltpu.VMEM((N_UNITS, N_DEV) + block, jnp.bfloat16), *halves,
            *[pltpu.VMEM((N_DEV, 4, LANES), F32)] * 3, pltpu.VMEM((N_DEV, TILE, LANES), F32), pltpu.VMEM((N_DEV, 1, LANES), F32),
            pltpu.VMEM((4, LANES), F32), pltpu.VMEM((TILE, LANES), F32), pltpu.VMEM((1, LANES), F32),
            pltpu.VMEM((1, LANES), F32), pltpu.VMEM((N_DEV, 1, LANES), F32),
            pltpu.VMEM((LANES, LANES), F32), pltpu.VMEM((D_MODEL, LANES), F32), pltpu.VMEM((2, 3, TILE, D_MODEL), F32),
            pltpu.SemaphoreType.DMA((N_UNITS + 1,)),
            pltpu.SemaphoreType.DMA((5,)), pltpu.SemaphoreType.DMA((5, N_UNITS)),
            pltpu.SemaphoreType.DMA((10,)),
            pltpu.SemaphoreType.DMA((TILE,)),
        ],
        compiler_params=pltpu.CompilerParams(
            has_side_effects=True, vmem_limit_bytes=52 * 2 ** 20, collective_id=1),
        name="dense_sums",
    )(*grads, *small, *experts)


def final_kernel(gs_v, rows, stat, *refs):
    (aw, iw, ow), expert_in, refs = refs[:3], refs[3:9], refs[9:]
    (aw_new, ar_new, ac_new, iw_new, ir_new, ic_new, ow_new, or_new, oc_new), refs = refs[:9], refs[9:]
    expert_out, updated, out_sem = refs[:6], refs[6:9], refs[9]

    outs = [pltpu.make_async_copy(a, b if k % 3 else b.at[0], out_sem.at[3 + k])
            for k, (a, b) in enumerate(zip(expert_in, expert_out))]
    for out in outs:
        out.start()

    scal = stat[N_DEV, 0:1, :]
    lane = lax.broadcasted_iota(jnp.int32, (1, LANES), 1)
    flipped = (jnp.transpose(rows[0:LANES, :]), jnp.transpose(rows[48:176, :]))
    for m in range(4):
        ar_new[m:m + 1, :] = flipped[0][0:1, N_DEV * m:N_DEV * m + N_DEV]
    ir_new[...] = flipped[1][0:1, 80:112]
    or_new[...] = flipped[1][0:1, 112:LANES]
    for m in range(6):
        row = m // 5
        row_total = over_cols(jnp.where(lane == m, scal, 0.0))
        if m == LAST:
            c_new = jnp.concatenate([stat[33, g:g + 1, :] for g in range(4)], axis=1)
            parts, row_total = stat[33, 4:5, 0:1], stat[33, 5:6, 0:1]
        else:
            c_new = jnp.concatenate([stat[TILE * (m % 5) + g, row:row + 1, :] for g in range(TILE)], axis=1)
            parts = sum(stat[TILE * (m % 5) + g, row + 2:row + 3, 0:1] for g in range(TILE))
        if m < 4:
            ac_new[m:m + 1, :] = c_new
        else:
            (ic_new, oc_new)[m - 4][...] = c_new
        w_sq = over_cols(jnp.where(lane == TILE + m, scal, 0.0))
        coeff = step_size(parts, w_sq, N_ROWS[m] * N_COLS[m])
        col_factor = lax.rsqrt(c_new)
        w = aw.at[m] if m < 4 else (iw, ow)[m - 4]
        for u in range(N_UNITS):
            if UNITS[u][0] != m:
                continue
            r_at, c_at = UNITS[u][1:]
            r_factor = lax.rsqrt(rows[ROW_AT[m] + r_at:ROW_AT[m] + r_at + BLK_R, 0:1] / (row_total / N_ROWS[m]))
            step = coeff * (gs_v[u] * r_factor * col_factor[:, c_at:c_at + BLK_C])
            part = (slice(r_at, r_at + BLK_R), slice(c_at, c_at + BLK_C))
            new = updated[0].at[m] if m < 4 else updated[m - 3]
            new[part] = w[part] - step
        if m >= 3:
            outs.append(pltpu.make_async_copy(updated[m - 3], (aw_new, iw_new, ow_new)[m - 3], out_sem.at[m - 3]))
            outs[-1].start()
    for out in outs:
        out.wait()


def final_update(sums):
    experts = [(1,) + shape if shape[0] > 1 else shape for shape in EXPERT_SHAPES]
    return pl.pallas_call(
        final_kernel,
        out_shape=shapes_of((4, N_DEV, D_MODEL), (4, N_DEV), (4, D_MODEL), (N_DEV, D_FF), (1, N_DEV), (1, D_FF), (16, D_MODEL), (1, 16),
                            (1, D_MODEL), *experts),
        in_specs=[VMEM] * 12,
        out_specs=[ANY, VMEM, VMEM] * 3 + [ANY] * 6,
        scratch_shapes=[*in_vmem(*[a.shape for a in sums[3:6]]), pltpu.SemaphoreType.DMA((9,))],
        compiler_params=pltpu.CompilerParams(vmem_limit_bytes=TILE * 2 ** 20),
        name="final_update",
    )(*sums)


def solution(mesh):
    dense_specs = (
        (P("dp"), P(None, "dp", None), P(None, "dp"), P()),
        (P("dp"), P("dp", None), P("dp"), P()),
        (P("dp"), P("dp", None), P("dp"), P()),
    )
    expert_specs = ((P("dp"), P("dp"), P("dp"), P("dp")),) * 2
    all_specs = dense_specs + expert_specs
    in_specs = tuple(part_spec for group in all_specs for part_spec in group)
    out_specs = tuple(part_spec for group in all_specs for part_spec in group[1:])

    def update_all(*arrays):
        (ag, aw, ar, ac, ig, iw, ir, ic, og, ow, orow, oc) = arrays[:12]
        grads = (ag.reshape(4, N_DEV, N_DEV, D_MODEL), ig.reshape(N_DEV, N_DEV, D_FF), og.reshape(N_DEV, 16, D_MODEL))
        sums = dense_sums(grads, (aw, iw, ow, ar, ir.reshape(1, N_DEV), orow.reshape(1, 16),
                                  ac, ic.reshape(1, D_FF), oc.reshape(1, D_MODEL)), arrays[12:])
        out = final_update(sums)
        return tuple(o.reshape(-1) if n in (4, 5, 7, TILE) else o for n, o in enumerate(out))

    return jax.shard_map(update_all, mesh=mesh, in_specs=in_specs, out_specs=out_specs, check_vma=False)
```
